768 devices in a mesh: gx: 96 (over x, z, core), gy: 8 (over y).
Axes of the slice: x: 4, y: 8, z: 12, core: 2. Of those that a mesh axis runs over, the one named last changes fastest.
Arguments:
- coarse_state: float32 [5, 3072, 2048], P(None, 'gx', 'gy'), may hold values from -6 to 6
- fine_state: float32 [768, 5, 32, 512], P(('gx', 'gy')), may hold values from -6 to 6
- slot_site: int32 [768, 2], P(('gx', 'gy')), may hold values from 0 to 7, as said below
- box_live: int32 [768], P(('gx', 'gy')), may hold values 0 or 1
Outputs:
- coarse_out: float32 [5, 3072, 2048], P(None, 'gx', 'gy')
- fine_out: float32 [768, 5, 32, 512], P(('gx', 'gy'))
The draws below stay inside these ranges and needn't reach their ends.
Inputs may be any that keep to these rules, and one draw needn't show every extreme that they name: `slot_site`: within each group of 8 devices that share a gx index, slots of the group and box positions of the group's coarse blocks are matched one to one; column 0 is the gy index of the block, column 1 the position number, 0 to 0.
All inputs are finite; a program needn't handle non-finite values. No bound on the sum of `box_live` on one device may be relied on, other than what follows from the above.
Results may differ from the reference program's by a relative error of at most 0.000088.
Values sent between devices are 32-bit elements; how exact they have to be, the bound alone decides.
A program may use at most 64 MiB of HBM per device.

```python
import jax
import jax.numpy as jnp
from jax import lax

NVAR = 5
CX = 32
CY = 32
NZ = 8
PATCH = 16
BOXES = 1
NX = 3072
NY = 256
N_GX = 96
N_GY = 8


def draw_slot_site(key, part):
    groups = NX // CX
    per_group = NY // CY * BOXES
    scores = jax.random.randint(key, (groups, per_group), 0, 1 << 20) * per_group + jnp.arange(per_group, dtype=jnp.int32)[None, :]
    matched = jnp.argsort(scores, axis=1).astype(jnp.int32)
    parent = matched // BOXES
    position = matched % BOXES
    return jnp.stack([parent, position], axis=-1).reshape(groups * per_group, 2).astype(jnp.int32)


def with_ends(array, rng, least, largest):
    place = [jax.random.randint(jax.random.fold_in(rng, axis), (), 0, length) for axis, length in enumerate(array.shape)]
    widest = array.shape.index(max(array.shape))
    next_to = place[:widest] + [(place[widest] + 1) % array.shape[widest]] + place[widest + 1:]
    return array.at[tuple(place)].set(least).at[tuple(next_to)].set(largest)


def shard_levels(stream_key, extent, cuts, low, high):
    level = 1.0
    for dim, blocks in cuts:
        heights = jax.random.uniform(jax.random.fold_in(jax.random.fold_in(stream_key, 6), dim), (blocks,), jnp.float32, low / len(cuts), high / len(cuts))
        level = level * jnp.repeat(jnp.exp(heights), extent[dim] // blocks).reshape((-1,) + (1,) * (len(extent) - 1 - dim))
    return level


def scatter_about(stream_key, dims, scale, reach, shards=(), kind=jnp.bfloat16):
    entries = scale * jax.random.normal(stream_key, dims, jnp.float32)
    if shards:
        entries = entries * shard_levels(stream_key, dims, shards, -0.22, 0.18)
    return jnp.clip(entries, -reach, reach).astype(kind)


def setup_inputs(seed: int = 0) -> dict:
    seeds = jax.random.split(jax.random.key(seed), 5)
    return {
        "coarse_state": scatter_about(seeds[0], (NVAR, NX, NY * NZ), 1.0, 6.0, ((1, 96), (2, 8)), jnp.float32),
        "fine_state": scatter_about(seeds[1], (N_GX * N_GY * BOXES, NVAR, 2 * PATCH, 4 * PATCH * NZ), 1.0, 6.0, ((0, 768),), jnp.float32),
        "slot_site": draw_slot_site(jax.random.fold_in(seeds[4], 71), 0),
        "box_live": with_ends((jax.random.randint(seeds[3], (N_GX * N_GY * BOXES,), 0, 2) < 1).astype(jnp.int32), jax.random.fold_in(seeds[3], 1), 0, 1),
    }


courant = 0.2
drift = (0.5, 0.3, 0.2)
sound_sq = 1.0
signal = (1.5, 1.3, 1.2)


def minmod(first, second):
    return jnp.maximum(jnp.minimum(first, second), 0.0) + jnp.minimum(jnp.maximum(first, second), 0.0)


def physical(values, direction):
    normal = values[1 + direction]
    pieces = []
    for member in range(5):
        summand = drift[direction] * values[member]
        if member == 0:
            summand = summand + normal
        if member == 1 + direction:
            summand = summand + values[4]
        if member == 4:
            summand = summand + sound_sq * normal
        pieces.append(summand)
    return jnp.stack(pieces)


def face_flux(values, axis_id, direction):
    length = values.shape[axis_id]
    left_cell = lax.slice_in_dim(values, 0, length - 2, axis=axis_id)
    centre = lax.slice_in_dim(values, 1, length - 1, axis=axis_id)
    right_cell = lax.slice_in_dim(values, 2, length, axis=axis_id)
    slopes = minmod(centre - left_cell, right_cell - centre)
    inner_len = length - 2
    left_face = lax.slice_in_dim(centre, 0, inner_len - 1, axis=axis_id) + 0.5 * lax.slice_in_dim(slopes, 0, inner_len - 1, axis=axis_id)
    right_face = lax.slice_in_dim(centre, 1, inner_len, axis=axis_id) - 0.5 * lax.slice_in_dim(slopes, 1, inner_len, axis=axis_id)
    return 0.5 * (physical(left_face, direction) + physical(right_face, direction)) - 0.5 * signal[direction] * (right_face - left_face)


def divergence(fluxes, axis_id):
    length = fluxes.shape[axis_id]
    return lax.slice_in_dim(fluxes, 1, length, axis=axis_id) - lax.slice_in_dim(fluxes, 0, length - 1, axis=axis_id)


def wrap_z(values):
    return jnp.concatenate([values[..., -2:], values, values[..., :2]], axis=-1)


def advance(padded, interior):
    flux_x = face_flux(padded[:, :, 2:-2, :], 1, 0)
    flux_y = face_flux(padded[:, 2:-2, :, :], 2, 1)
    flux_z = face_flux(wrap_z(interior), 3, 2)
    change = divergence(flux_x, 1) + divergence(flux_y, 2) + divergence(flux_z, 3)
    return interior - courant * change, flux_x, flux_y


def inject(fine, window):
    spread = jnp.repeat(jnp.repeat(jnp.repeat(window, 2, axis=1), 2, axis=2), 2, axis=3)
    return spread.at[:, 2:2 + 2 * PATCH, 2:2 + 2 * PATCH, :].set(fine)


def coarsen_face(fluxes):
    shape_now = fluxes.shape
    return fluxes.reshape(shape_now[0], shape_now[1] // 2, 2, shape_now[2] // 2, 2).mean(axis=(2, 4))


def fine_cycle(fine, early, later):
    first, flux_x_one, flux_y_one = advance(inject(fine, early), fine)
    second, flux_x_two, flux_y_two = advance(inject(first, 0.5 * (early + later)), first)
    edge = 2 * PATCH
    registers = [
        0.5 * (coarsen_face(flux_x_one[:, 0]) + coarsen_face(flux_x_two[:, 0])),
        0.5 * (coarsen_face(flux_x_one[:, edge]) + coarsen_face(flux_x_two[:, edge])),
        0.5 * (coarsen_face(flux_y_one[:, :, 0]) + coarsen_face(flux_y_two[:, :, 0])),
        0.5 * (coarsen_face(flux_y_one[:, :, edge]) + coarsen_face(flux_y_two[:, :, edge])),
    ]
    shape_now = second.shape
    average = second.reshape(shape_now[0], shape_now[1] // 2, 2, shape_now[2] // 2, 2, shape_now[3] // 2, 2).mean(axis=(2, 4, 6))
    return second, jnp.concatenate([average, jnp.stack(registers, axis=1)], axis=1)


def reference(coarse_state, fine_state, slot_site, box_live):
    coarse_state = coarse_state.reshape(NVAR, NX, NY, NZ)
    fine_state = fine_state.reshape(fine_state.shape[0], NVAR, 2 * PATCH, 2 * PATCH, 2 * NZ)
    padded = jnp.pad(coarse_state, ((0, 0), (2, 2), (2, 2), (0, 0)), mode="wrap")
    coarse_new, flux_x, flux_y = advance(padded, coarse_state)
    per_row = CY // 32
    per_group = N_GY * BOXES
    slot_ids = jnp.arange(fine_state.shape[0], dtype=jnp.int32)
    group = slot_ids // per_group
    parent = slot_site[:, 0].astype(jnp.int32)
    position = slot_site[:, 1].astype(jnp.int32)
    anchor_x = (group * CX + 32 * (position // per_row) + 8).astype(jnp.int32)
    anchor_y = (parent * CY + 32 * (position % per_row) + 8).astype(jnp.int32)
    live = box_live[((group * N_GY + parent) * BOXES + position).astype(jnp.int32)].astype(coarse_state.dtype)
    nought = jnp.zeros((), jnp.int32)

    def one_box(items):
        fine, start_x, start_y = items
        early = lax.dynamic_slice(coarse_state, (nought, start_x - 1, start_y - 1, nought), (NVAR, PATCH + 2, PATCH + 2, NZ))
        later = lax.dynamic_slice(coarse_new, (nought, start_x - 1, start_y - 1, nought), (NVAR, PATCH + 2, PATCH + 2, NZ))
        return fine_cycle(fine, early, later)

    fine_out, payload = lax.map(one_box, (fine_state, anchor_x, anchor_y))
    offsets = jnp.arange(PATCH, dtype=jnp.int32)
    rows_x = anchor_x[:, None] + offsets[None, :]
    rows_y = anchor_y[:, None] + offsets[None, :]
    present = live > 0
    covered = coarse_new[:, rows_x[:, :, None], rows_y[:, None, :], :]
    average = jnp.moveaxis(payload[:, :, :PATCH], 0, 1)
    result = coarse_new.at[:, rows_x[:, :, None], rows_y[:, None, :], :].set(jnp.where(present[None, :, None, None, None], average, covered))
    weight = courant * live[None, :, None, None]

    def register(index):
        return jnp.moveaxis(payload[:, :, PATCH + index], 0, 1)

    low_x = anchor_x[:, None]
    high_x = low_x + PATCH
    low_y = anchor_y[:, None]
    high_y = low_y + PATCH
    result = result.at[:, low_x - 1, rows_y, :].add(weight * (flux_x[:, low_x, rows_y, :] - register(0)))
    result = result.at[:, high_x, rows_y, :].add(weight * (register(1) - flux_x[:, high_x, rows_y, :]))
    result = result.at[:, rows_x, low_y - 1, :].add(weight * (flux_y[:, rows_x, low_y, :] - register(2)))
    result = result.at[:, rows_x, high_y, :].add(weight * (register(3) - flux_y[:, rows_x, high_y, :]))
    fine_shape = fine_out.shape
    return result.reshape(NVAR, NX, NY * NZ), fine_out.reshape(fine_shape[0], NVAR, 2 * PATCH, fine_shape[3] * fine_shape[4])
```

```python
import jax
import jax.numpy as jnp
from jax import lax
from jax.experimental import pallas as pl
from jax.experimental.pallas import tpu as pltpu
from jax.sharding import PartitionSpec as P

NV = 5
GY = 8
courant = 0.2
drift = (0.5, 0.3, 0.2)
signal = (1.5, 1.3, 1.2)
MESH = pl.DeviceIdType.MESH
F32 = jnp.float32


def iota(shape, dim):
    return lax.broadcasted_iota(jnp.int32, shape, dim)


def up(x, n, axis):
    return pltpu.roll(x, x.shape[axis] - n, axis)


def down(x, n, axis):
    return pltpu.roll(x, n, axis)


def z_up(x, depth):
    last = iota(x.shape, 1) % depth == depth - 1
    return jnp.where(last, pltpu.roll(x, depth - 1, 1), pltpu.roll(x, 127, 1))


def z_down(x, depth):
    first = iota(x.shape, 1) % depth == 0
    return jnp.where(first, pltpu.roll(x, 129 - depth, 1), pltpu.roll(x, 1, 1))


def minmod(a, b):
    return jnp.maximum(jnp.minimum(a, b), 0.0) + jnp.minimum(jnp.maximum(a, b), 0.0)


def face_fluxes(q, d, ahead, behind):
    plus = 0.5 * (drift[d] + signal[d])
    minus = 0.5 * (drift[d] - signal[d])
    left, right = [], []
    for v in q:
        diff = ahead(v) - v
        half = 0.5 * minmod(behind(diff), diff)
        left.append(v + half)
        right.append(v - half)

    def side(s, coef):
        vn = 0.5 * s[1 + d]
        out = [coef * x for x in s]
        out[0] = out[0] + vn
        out[4] = out[4] + vn
        out[1 + d] = out[1 + d] + 0.5 * s[4]
        return out

    a, b = side(left, plus), side(right, minus)
    return [x + ahead(y) for x, y in zip(a, b)]


def z_pass(q_ref, out_ref, width, depth):
    for t in range(width // 128):
        lanes = pl.ds(128 * t, 128)
        q = [q_ref[m, 0:32, lanes] for m in range(NV)]
        f = face_fluxes(q, 2, lambda x: z_up(x, depth), lambda x: z_down(x, depth))
        for m in range(NV):
            out_ref[m, :, lanes] = f[m] - z_down(f[m], depth)


def x_pass(q_ref, out_ref, width, keep):
    for t in range(width // 128):
        lanes = pl.ds(128 * t, 128)
        q = [q_ref[m, :, lanes] for m in range(NV)]
        f = face_fluxes(q, 0, lambda x: up(x, 1, 0), lambda x: down(x, 1, 0))
        for m in range(NV):
            low = down(f[m], 1, 0)
            out_ref[m, :, lanes] = (f[m] - low)[0:32]
            keep(m, lanes, f[m], low)


def y_pass(q_ref, width, depth, emit, keep):
    for r in range(4):
        rows = pl.ds(8 * r, 8)
        q = [q_ref[m, rows, :] for m in range(NV)]
        f = face_fluxes(q, 1, lambda x: up(x, depth, 1), lambda x: down(x, depth, 1))
        for m in range(NV):
            low = down(f[m], depth, 1)
            keep(m, r, f[m], low)
            emit(m, r, q[m][:, 0:width], (f[m] - low)[:, 0:width])


def dot(a, b):
    return jnp.dot(a, b, precision=lax.Precision.HIGHEST, preferred_element_type=F32)


def kernel(
    coarse, fine, site_ref, live_ref, coarse_out, fine_out,
    cq, fq, cz, cx, cn, fz, fx, cflx, cfly, xf, yf, ps,
    spread_x, spread_y, gather_x, gather_y, ring, mids, pieces, stage, order, arrived,
    hxs, hxr, hys, hyr,
    in_sem, out_sem, ring_s, ring_r, mid_s, mid_r, one_s, one_r, two_s, two_r, hal_s, hal_r,
):
    gx, gy = lax.axis_index("gx"), lax.axis_index("gy")
    ngx = lax.axis_size("gx")
    site = site_ref[0, 0]
    live = live_ref[0]

    load_c = pltpu.make_async_copy(coarse, cq.at[:, 0:32, 0:256], in_sem.at[0])
    load_f = pltpu.make_async_copy(fine, fq.at[:, 0:32, 0:512], in_sem.at[1])
    load_c.start()
    load_f.start()
    barrier = pltpu.get_barrier_semaphore()
    gx_lo, gx_hi = lax.rem(gx + ngx - 1, ngx), lax.rem(gx + 1, ngx)
    for g in (gx_lo, gx_hi):
        pl.semaphore_signal(barrier, inc=1, device_id=(g, gy), device_id_type=MESH)
    far = (4, 3, 5, 2, 6, 1, 7)
    peers = [lax.rem(gy + k, GY) for k in far]
    for p in peers:
        pl.semaphore_signal(barrier, inc=1, device_id=(gx, p), device_id_type=MESH)

    k, o = iota((128, 512), 0), iota((128, 512), 1)
    spread_x[...] = jnp.where(k == (o // 32) * 8 + (o % 16) // 2, 1.0, 0.0)
    k, o = iota((256, 128), 0), iota((256, 128), 1)
    hit = (k % 8 == (o % 16) // 2) & (((k < 128) & (o >= 96)) | ((k >= 128) & (o < 32)))
    spread_y[...] = jnp.where(hit, 1.0, 0.0)
    k, o = iota((512, 128), 0), iota((512, 128), 1)
    gather_x[...] = jnp.where(o == (k // 32) * 8 + (k % 16) // 2, 0.125, 0.0)
    k, o = iota((128, 128), 0), iota((128, 128), 1)
    gather_y[...] = jnp.where((k >= 112) & ((k % 16) // 2 == o % 8), 0.125, 0.0)
    pick_low = jnp.where(k == 56 + o % 8, 1.0, 0.0)
    pick_high = jnp.where(k == 64 + o % 8, 1.0, 0.0)

    cq[:, 32:40, :] = jnp.zeros((NV, 8, 384), F32)
    cq[:, 0:32, 256:384] = jnp.zeros((NV, 32, 128), F32)
    fq[:, 32:40, :] = jnp.zeros((NV, 8, 640), F32)
    xf[...] = jnp.zeros((16, 512), F32)

    lane16 = iota((16, 128), 1)
    own = lane16 // 8 == iota((16, 128), 0)

    def put_ring(dst, get):
        for m in range(NV):
            for face, row in ((0, 7), (1, 24)):
                first, second = get(m, row, row + 1, 0), get(m, row, row + 1, 1)
                both = jnp.where(
                    iota((1, 128), 1) < 64, pltpu.roll(first, 64, 1), pltpu.roll(second, 64, 1)
                )
                dst[gy, 5 * face + m : 5 * face + m + 1, :] = both
        for face, pick in ((2, pick_low), (3, pick_high)):
            cols = jnp.concatenate([get(m, 8, 24, face - 2) for m in range(NV)], axis=0)
            copies = dot(cols, pick)
            for m in range(NV):
                part = jnp.where(own, copies[16 * m : 16 * m + 16], 0.0)
                dst[gy, 5 * face + m : 5 * face + m + 1, :] = jnp.sum(part, axis=0, keepdims=True)

    load_c.wait()
    ring[gy, 16:24, :] = jnp.full((8, 128), site, jnp.int32).astype(F32)
    put_ring(ring, lambda m, a, b, t: cq[m, a:b, 128 * t : 128 * t + 128])
    for m in range(NV):
        hxs[0, 2 * m : 2 * m + 2, :] = cq[m, 0:2, 0:256]
        hxs[1, 2 * m : 2 * m + 2, :] = cq[m, 30:32, 0:256]
    lane8 = iota((8, 128), 1)
    for side, tile, base in ((0, 0, 0), (1, 1, 112)):
        for g in range(3):
            acc = jnp.zeros((8, 128), F32)
            for n in range(8 * g, min(8 * g + 8, 20)):
                block = cq[n // 4, 8 * (n % 4) : 8 * (n % 4) + 8, 128 * tile : 128 * tile + 128]
                moved = pltpu.roll(block, (16 * (n % 8) - base) % 128, 1) if (16 * (n % 8) - base) % 128 else block
                acc = jnp.where(lane8 // 16 == n % 8, moved, acc)
            hys[side, g] = acc

    def spread(buf, sends, recvs):
        out = []
        for i, p in enumerate(peers):
            c = pltpu.make_async_remote_copy(
                src_ref=buf.at[gy], dst_ref=buf.at[gy], send_sem=sends.at[i], recv_sem=recvs.at[gy],
                device_id=(gx, p), device_id_type=MESH,
            )
            c.start()
            out.append(c)
        return out

    def received(buf, sends, recvs):
        for i, k in enumerate(far):
            src = lax.rem(gy + GY - k, GY)
            pltpu.make_async_remote_copy(
                src_ref=buf.at[src], dst_ref=buf.at[src], send_sem=sends.at[i], recv_sem=recvs.at[src],
                device_id=(gx, src), device_id_type=MESH,
            ).wait_recv()

    pl.semaphore_wait(barrier, 9)
    pending = spread(ring, ring_s, ring_r)

    def coarse_keep_x(m, lanes, f, low):
        cflx[m, 0, :, lanes] = f[0:8]
        cflx[m, 1, :, lanes] = low[24:32]

    def coarse_keep_y(m, r, f, low):
        if r in (1, 2):
            cfly[m, 0, 8 * (r - 1) : 8 * r, :] = f[:, 0:128]
            cfly[m, 1, 8 * (r - 1) : 8 * r, :] = low[:, 128:256]

    def coarse_emit(m, r, q, div):
        rows = pl.ds(8 * r, 8)
        cn[m, rows, :] = q - courant * (cx[m, rows, :] + cz[m, rows, :] + div)

    z_pass(cq, cz, 256, 8)
    x_pass(cq, cx, 256, coarse_keep_x)
    y_pass(cq, 256, 8, coarse_emit, coarse_keep_y)
    put_ring(
        mids,
        lambda m, a, b, t: 0.5
        * (cq[m, a:b, 128 * t : 128 * t + 128] + cn[m, a:b, 128 * t : 128 * t + 128]),
    )
    pending += spread(mids, mid_s, mid_r)

    gy_lo, gy_hi = lax.rem(gy + GY - 1, GY), lax.rem(gy + 1, GY)
    for i, (src, dst, where) in enumerate(
        (
            (hxs.at[0], hxr.at[0], (gx_lo, gy)),
            (hxs.at[1], hxr.at[1], (gx_hi, gy)),
            (hys.at[0], hyr.at[0], (gx, gy_lo)),
            (hys.at[1], hyr.at[1], (gx, gy_hi)),
        )
    ):
        c = pltpu.make_async_remote_copy(
            src_ref=src, dst_ref=dst, send_sem=hal_s.at[i], recv_sem=hal_r.at[i],
            device_id=where, device_id_type=MESH,
        )
        c.start()
        pending.append(c)
    halo = pending[-4:]

    site_v = jnp.full((24, 128), site, jnp.int32)
    row32 = iota((32, 128), 0)
    mine = iota((32, 128), 1) // 8 == row32 // 2

    def ghosts(buf):
        got = jnp.zeros((24, 128), F32)
        for s in range(GY):
            got = jnp.where(site_v == s, buf[s], got)
        wide = dot(got[0:16], spread_x[...])
        lows = jnp.concatenate([jnp.where(mine, got[10 + m : 11 + m], 0.0) for m in range(NV)], axis=0)
        highs = jnp.concatenate([jnp.where(mine, got[15 + m : 16 + m], 0.0) for m in range(NV)], axis=0)
        side = dot(jnp.concatenate([lows, highs], axis=1), spread_y[...])
        edge = iota((8, 512), 0) < 4
        for m in range(NV):
            fq[m, 32:40, 0:512] = jnp.where(edge, wide[5 + m : 6 + m], wide[m : m + 1])
            fq[m, 0:32, 512:640] = side[32 * m : 32 * m + 32]

    def fine_step(first):
        def keep_x(m, lanes, f, low):
            if first:
                xf[m : m + 1, lanes] = f[39:40]
                xf[5 + m : 6 + m, lanes] = f[31:32]
            else:
                xf[m : m + 1, lanes] += f[39:40]
                xf[5 + m : 6 + m, lanes] += f[31:32]

        def keep_y(m, r, f, low):
            at = 64 * m + 8 * r
            if first:
                yf[at : at + 8, :] = f[:, 512:640]
                yf[at + 32 : at + 40, :] = f[:, 384:512]
            else:
                yf[at : at + 8, :] += f[:, 512:640]
                yf[at + 32 : at + 40, :] += f[:, 384:512]

        def emit(m, r, q, div):
            rows = pl.ds(8 * r, 8)
            new = q - courant * (fx[m, rows, :] + fz[m, rows, :] + div)
            fq[m, rows, 0:512] = new
            if not first:
                for t in range(4):
                    ps[t, 32 * m + 8 * r : 32 * m + 8 * r + 8, :] = new[:, 128 * t : 128 * t + 128]

        x_pass(fq, fx, 512, keep_x)
        y_pass(fq, 512, 16, emit, keep_y)

    load_f.wait()
    z_pass(fq, fz, 512, 16)
    received(ring, ring_s, ring_r)
    ghosts(ring)
    fine_step(True)
    z_pass(fq, fz, 512, 16)
    received(mids, mid_s, mid_r)
    ghosts(mids)
    fine_step(False)
    store_f = pltpu.make_async_copy(fq.at[:, 0:32, 0:512], fine_out, out_sem.at[0])
    store_f.start()

    pairs = jnp.concatenate(
        [ps[t, pl.ds(0, 80, stride=2), :] + ps[t, pl.ds(1, 80, stride=2), :] for t in range(4)], axis=1
    )
    means = dot(jnp.concatenate([pairs, xf[...]], axis=0), gather_x[...])
    for a in range(6):
        pieces[a] = means[16 * a : 16 * a + 16]
    cols = dot(yf[pl.ds(0, 160, stride=2), :] + yf[pl.ds(1, 160, stride=2), :], gather_y[...])
    acc = jnp.zeros((16, 128), F32)
    for n in range(10):
        acc = jnp.where(lane16 // 8 == n, cols[16 * n : 16 * n + 16], acc)
    pieces[6] = acc

    def exchange_one(i, p, s):
        return pltpu.make_async_remote_copy(
            src_ref=pieces.at[p], dst_ref=stage.at[s], send_sem=one_s.at[i], recv_sem=one_r.at[s],
            device_id=(gx, p), device_id_type=MESH,
        )

    def exchange_two(i, p, s):
        return pltpu.make_async_remote_copy(
            src_ref=order.at[p], dst_ref=arrived.at[s], send_sem=two_s.at[i], recv_sem=two_r.at[s],
            device_id=(gx, p), device_id_type=MESH,
        )

    for i, p in enumerate(peers):
        @pl.when(p != GY - 1)
        def _():
            exchange_one(i, p, gy).start()

    stage[gy] = pieces[gy]

    for c in halo:
        c.wait_recv()
    for m in range(NV):
        two = jnp.concatenate([hxr[0, 2 * m : 2 * m + 2, :], jnp.zeros((4, 256), F32), hxr[1, 2 * m : 2 * m + 2, :]], axis=0)
        cq[m, 32:40, 0:256] = two
        for r in range(4):
            n = 4 * m + r
            high = pltpu.roll(hyr[0, n // 8], (-16 * (n % 8)) % 128, 1) if n % 8 else hyr[0, n // 8]
            low = pltpu.roll(hyr[1, n // 8], (112 - 16 * (n % 8)) % 128, 1) if n % 8 != 7 else hyr[1, n // 8]
            cq[m, 8 * r : 8 * r + 8, 256:384] = jnp.where(
                lane8 < 16, high, jnp.where(lane8 >= 112, low, 0.0)
            )
    x_pass(cq, cx, 256, coarse_keep_x)
    y_pass(cq, 256, 8, coarse_emit, coarse_keep_y)

    weight = jnp.full((16, 128), live, jnp.int32).astype(F32) * courant
    w8 = weight[0:8]
    present = jnp.full((16, 128), live, jnp.int32) > 0
    row8 = iota((8, 128), 0)

    @pl.when(gy != GY - 1)
    def _():
        for i, k in enumerate(far):
            exchange_one(i, gy, lax.rem(gy + GY - k, GY)).wait_recv()
        tags = [jnp.broadcast_to(ring[s, 23:24, :], (16, 128)) for s in range(GY)]
        for d in range(GY):
            acc = jnp.zeros((16, 128), F32)
            for s in range(GY):
                acc = jnp.where(tags[s] == float(d), stage[s], acc)
            order[d] = acc
        for i, p in enumerate(peers):
            exchange_two(i, p, gy).start()
        arrived[gy] = order[gy]

    for i, k in enumerate(far):
        src = lax.rem(gy + GY - k, GY)

        @pl.when(src != GY - 1)
        def _():
            exchange_two(i, src, src).wait_recv()

    for m in range(NV):
        mean = pltpu.roll(arrived[m], 64, 1)
        left = cn[m, 8:24, 0:128]
        right = cn[m, 8:24, 128:256]
        left = jnp.where(present & (lane16 >= 64), mean, left)
        right = jnp.where(present & (lane16 < 64), mean, right)
        low = pltpu.roll(arrived[6], (56 - 16 * m) % 128, 1)
        high = pltpu.roll(arrived[6], (56 - 16 * m) % 128, 1)
        left = left + jnp.where(lane16 // 8 == 7, weight * (cfly[m, 0] - low), 0.0)
        right = right + jnp.where(lane16 // 8 == 8, weight * (high - cfly[m, 1]), 0.0)
        cn[m, 8:24, 0:128] = left
        cn[m, 8:24, 128:256] = right
        low = jnp.broadcast_to(pltpu.roll(arrived[5, m : m + 1, :], 64, 1), (8, 128))
        high = jnp.broadcast_to(pltpu.roll(arrived[5, 5 + m : 6 + m, :], 64, 1), (8, 128))
        for t in range(2):
            lanes = pl.ds(128 * t, 128)
            inside = lane8 >= 64 if t == 0 else lane8 < 64
            cn[m, 0:8, lanes] += jnp.where(inside & (row8 == 7), w8 * (cflx[m, 0, :, lanes] - low), 0.0)
            cn[m, 24:32, lanes] += jnp.where(inside & (row8 == 0), w8 * (high - cflx[m, 1, :, lanes]), 0.0)

    store_c = pltpu.make_async_copy(cn, coarse_out, out_sem.at[1])
    store_c.start()
    for c in pending:
        c.wait_send()
    for i, p in enumerate(peers):
        @pl.when(p != GY - 1)
        def _():
            exchange_one(i, p, gy).wait_send()

    @pl.when(gy != GY - 1)
    def _():
        for i, p in enumerate(peers):
            exchange_two(i, p, gy).wait_send()

    store_f.wait()
    store_c.wait()


def shards(coarse_state, fine_state, slot_site, box_live):
    dma = pltpu.SemaphoreType.DMA
    vm = lambda *s: pltpu.VMEM(s, F32)
    coarse_out, fine_out = pl.pallas_call(
        kernel,
        out_shape=(
            jax.ShapeDtypeStruct((NV, 32, 256), F32),
            jax.ShapeDtypeStruct((NV, 32, 512), F32),
        ),
        in_specs=[
            pl.BlockSpec(memory_space=pl.ANY),
            pl.BlockSpec(memory_space=pl.ANY),
            pl.BlockSpec(memory_space=pltpu.SMEM),
            pl.BlockSpec(memory_space=pltpu.SMEM),
        ],
        out_specs=[pl.BlockSpec(memory_space=pl.ANY)] * 2,
        scratch_shapes=[
            vm(NV, 40, 384), vm(NV, 40, 640),
            vm(NV, 32, 256), vm(NV, 32, 256), vm(NV, 32, 256),
            vm(NV, 32, 512), vm(NV, 32, 512),
            vm(NV, 2, 8, 256), vm(NV, 2, 16, 128),
            vm(16, 512), vm(320, 128), vm(4, 160, 128),
            vm(128, 512), vm(256, 128), vm(512, 128), vm(128, 128),
            vm(GY, 24, 128), vm(GY, 24, 128),
            vm(GY, 16, 128), vm(GY, 16, 128), vm(GY, 16, 128), vm(GY, 16, 128),
            vm(2, 16, 256), vm(2, 16, 256), vm(2, 3, 8, 128), vm(2, 3, 8, 128),
            dma((2,)), dma((2,)),
            dma((7,)), dma((8,)), dma((7,)), dma((8,)), dma((7,)), dma((8,)), dma((7,)), dma((8,)),
            dma((4,)), dma((4,)),
        ],
        compiler_params=pltpu.CompilerParams(collective_id=0, has_side_effects=True),
        name="amr_step",
    )(coarse_state, fine_state.reshape(NV, 32, 512), slot_site, box_live)
    return coarse_out, fine_out.reshape(1, NV, 32, 512)


def solution(mesh):
    return jax.shard_map(
        shards,
        mesh=mesh,
        in_specs=(
            P(None, "gx", "gy"),
            P(("gx", "gy"), None, None, None),
            P(("gx", "gy"), None),
            P(("gx", "gy")),
        ),
        out_specs=(P(None, "gx", "gy"), P(("gx", "gy"), None, None, None)),
        check_vma=False,
    )
```

```python
import jax
import jax.numpy as jnp
from jax import lax
from jax.experimental import pallas as pl
from jax.experimental.pallas import tpu as pltpu
from jax.sharding import PartitionSpec as P

NV = 5
GY = 8
courant = 0.2
drift = (0.5, 0.3, 0.2)
signal = (1.5, 1.3, 1.2)
MESH = pl.DeviceIdType.MESH
F32 = jnp.float32


def iota(shape, dim):
    return lax.broadcasted_iota(jnp.int32, shape, dim)


def up(x, n, axis):
    return pltpu.roll(x, x.shape[axis] - n, axis)


def down(x, n, axis):
    return pltpu.roll(x, n, axis)


def z_up(x, depth):
    last = iota(x.shape, 1) % depth == depth - 1
    return jnp.where(last, pltpu.roll(x, depth - 1, 1), pltpu.roll(x, 127, 1))


def z_down(x, depth):
    first = iota(x.shape, 1) % depth == 0
    return jnp.where(first, pltpu.roll(x, 129 - depth, 1), pltpu.roll(x, 1, 1))


def minmod(a, b):
    return jnp.maximum(jnp.minimum(a, b), 0.0) + jnp.minimum(jnp.maximum(a, b), 0.0)


def face_fluxes(q, d, ahead, behind):
    plus = 0.5 * (drift[d] + signal[d])
    minus = 0.5 * (drift[d] - signal[d])
    left, right = [], []
    for v in q:
        diff = ahead(v) - v
        half = 0.5 * minmod(behind(diff), diff)
        left.append(v + half)
        right.append(v - half)

    def side(s, coef):
        vn = 0.5 * s[1 + d]
        out = [coef * x for x in s]
        out[0] = out[0] + vn
        out[4] = out[4] + vn
        out[1 + d] = out[1 + d] + 0.5 * s[4]
        return out

    a, b = side(left, plus), side(right, minus)
    return [x + ahead(y) for x, y in zip(a, b)]


def z_pass(q_ref, out_ref, width, depth):
    for t in range(width // 128):
        lanes = pl.ds(128 * t, 128)
        q = [q_ref[m, 0:32, lanes] for m in range(NV)]
        f = face_fluxes(q, 2, lambda x: z_up(x, depth), lambda x: z_down(x, depth))
        for m in range(NV):
            out_ref[m, :, lanes] = f[m] - z_down(f[m], depth)


def x_pass(q_ref, out_ref, width, keep):
    for t in range(width // 128):
        lanes = pl.ds(128 * t, 128)
        q = [q_ref[m, :, lanes] for m in range(NV)]
        f = face_fluxes(q, 0, lambda x: up(x, 1, 0), lambda x: down(x, 1, 0))
        for m in range(NV):
            low = down(f[m], 1, 0)
            out_ref[m, :, lanes] = (f[m] - low)[0:32]
            keep(m, lanes, f[m], low)


def y_pass(q_ref, width, depth, emit, keep):
    for r in range(4):
        rows = pl.ds(8 * r, 8)
        q = [q_ref[m, rows, :] for m in range(NV)]
        f = face_fluxes(q, 1, lambda x: up(x, depth, 1), lambda x: down(x, depth, 1))
        for m in range(NV):
            low = down(f[m], depth, 1)
            keep(m, r, f[m], low)
            emit(m, r, q[m][:, 0:width], (f[m] - low)[:, 0:width])


def dot(a, b):
    return jnp.dot(a, b, precision=lax.Precision.HIGHEST, preferred_element_type=F32)


def kernel(
    coarse, fine, site_ref, live_ref, cn, fine_out,
    cq, fq, cz, cx, fz, fx, cflx, cfly, xf, yf, ps,
    spread_x, spread_y, gather_x, gather_y, ring, mids, pieces, stage, order, arrived,
    hxs, hxr, hys, hyr,
    in_sem, ring_s, ring_r, mid_s, mid_r, one_s, one_r, two_s, two_r, hal_s, hal_r, ready,
):
    gx, gy = lax.axis_index("gx"), lax.axis_index("gy")
    ngx = lax.axis_size("gx")
    site = site_ref[0, 0]
    live = live_ref[0]

    load_c = pltpu.make_async_copy(coarse, cq.at[:, 0:32, 0:256], in_sem.at[0])
    load_f = pltpu.make_async_copy(fine, fq.at[:, 0:32, 0:512], in_sem.at[1])
    load_c.start()
    load_f.start()
    barrier = pltpu.get_barrier_semaphore()
    gx_lo, gx_hi = lax.rem(gx + ngx - 1, ngx), lax.rem(gx + 1, ngx)
    odd = lax.rem(gx, 2)

    @pl.when(odd == 0)
    def _():
        for g in (gx_lo, gx_hi):
            pl.semaphore_signal(barrier, inc=1, device_id=(g, gy), device_id_type=MESH)

    far = (4, 3, 5, 2, 6, 1, 7)
    peers = [lax.rem(gy + k, GY) for k in far]
    for p in peers:
        pl.semaphore_signal(barrier, inc=1, device_id=(gx, p), device_id_type=MESH)

    k, o = iota((128, 512), 0), iota((128, 512), 1)
    spread_x[...] = jnp.where(k == (o // 32) * 8 + (o % 16) // 2, 1.0, 0.0)
    k, o = iota((256, 128), 0), iota((256, 128), 1)
    hit = (k % 8 == (o % 16) // 2) & (((k < 128) & (o >= 96)) | ((k >= 128) & (o < 32)))
    spread_y[...] = jnp.where(hit, 1.0, 0.0)
    k, o = iota((512, 128), 0), iota((512, 128), 1)
    gather_x[...] = jnp.where(o == (k // 32) * 8 + (k % 16) // 2, 0.125, 0.0)
    k, o = iota((128, 128), 0), iota((128, 128), 1)
    gather_y[...] = jnp.where((k >= 112) & ((k % 16) // 2 == o % 8), 0.125, 0.0)
    pick_low = jnp.where(k == 56 + o % 8, 1.0, 0.0)
    pick_high = jnp.where(k == 64 + o % 8, 1.0, 0.0)

    cq[:, 32:40, :] = jnp.zeros((NV, 8, 384), F32)
    cq[:, 0:32, 256:384] = jnp.zeros((NV, 32, 128), F32)
    fq[:, 32:40, :] = jnp.zeros((NV, 8, 640), F32)
    xf[...] = jnp.zeros((16, 512), F32)

    lane16 = iota((16, 128), 1)
    own = lane16 // 8 == iota((16, 128), 0)

    def put_ring(dst, get):
        for m in range(NV):
            for face, row in ((0, 7), (1, 24)):
                first, second = get(m, row, row + 1, 0), get(m, row, row + 1, 1)
                both = jnp.where(
                    iota((1, 128), 1) < 64, pltpu.roll(first, 64, 1), pltpu.roll(second, 64, 1)
                )
                dst[gy, 5 * face + m : 5 * face + m + 1, :] = both
        for face, pick in ((2, pick_low), (3, pick_high)):
            cols = jnp.concatenate([get(m, 8, 24, face - 2) for m in range(NV)], axis=0)
            copies = dot(cols, pick)
            for m in range(NV):
                part = jnp.where(own, copies[16 * m : 16 * m + 16], 0.0)
                dst[gy, 5 * face + m : 5 * face + m + 1, :] = jnp.sum(part, axis=0, keepdims=True)

    load_c.wait()
    ring[gy, 16:24, :] = jnp.full((8, 128), site, jnp.int32).astype(F32)
    put_ring(ring, lambda m, a, b, t: cq[m, a:b, 128 * t : 128 * t + 128])
    for m in range(NV):
        hxs[0, 2 * m : 2 * m + 2, :] = cq[m, 0:2, 0:256]
        hxs[1, 2 * m : 2 * m + 2, :] = cq[m, 30:32, 0:256]
    lane8 = iota((8, 128), 1)
    for side, tile, base in ((0, 0, 0), (1, 1, 112)):
        for g in range(3):
            acc = jnp.zeros((8, 128), F32)
            for n in range(8 * g, min(8 * g + 8, 20)):
                block = cq[n // 4, 8 * (n % 4) : 8 * (n % 4) + 8, 128 * tile : 128 * tile + 128]
                moved = pltpu.roll(block, (16 * (n % 8) - base) % 128, 1) if (16 * (n % 8) - base) % 128 else block
                acc = jnp.where(lane8 // 16 == n % 8, moved, acc)
            hys[side, g] = acc

    def spread(buf, sends, recvs):
        out = []
        for i, p in enumerate(peers):
            c = pltpu.make_async_remote_copy(
                src_ref=buf.at[gy], dst_ref=buf.at[gy], send_sem=sends.at[i], recv_sem=recvs.at[gy],
                device_id=(gx, p), device_id_type=MESH,
            )
            c.start()
            out.append(c)
        return out

    def received(buf, sends, recvs):
        for i, k in enumerate(far):
            src = lax.rem(gy + GY - k, GY)
            pltpu.make_async_remote_copy(
                src_ref=buf.at[src], dst_ref=buf.at[src], send_sem=sends.at[i], recv_sem=recvs.at[src],
                device_id=(gx, src), device_id_type=MESH,
            ).wait_recv()

    gy_lo, gy_hi = lax.rem(gy + GY - 1, GY), lax.rem(gy + 1, GY)
    halo = [
        pltpu.make_async_remote_copy(
            src_ref=src, dst_ref=dst, send_sem=hal_s.at[i], recv_sem=hal_r.at[i],
            device_id=where, device_id_type=MESH,
        )
        for i, (src, dst, where) in enumerate(
            (
                (hxs.at[0], hxr.at[0], (gx_lo, gy)),
                (hxs.at[1], hxr.at[1], (gx_hi, gy)),
                (hys.at[0], hyr.at[0], (gx, gy_lo)),
                (hys.at[1], hyr.at[1], (gx, gy_hi)),
            )
        )
    ]
    pl.semaphore_wait(barrier, 7 + 2 * odd)

    @pl.when(odd == 1)
    def _():
        for g in (gx_lo, gx_hi):
            pl.semaphore_signal(ready, inc=1, device_id=(g, gy), device_id_type=MESH)
        for c in halo[:2]:
            c.start()

    pending = spread(ring, ring_s, ring_r)

    def coarse_keep_x(m, lanes, f, low):
        cflx[m, 0, :, lanes] = f[0:8]
        cflx[m, 1, :, lanes] = low[24:32]

    def coarse_keep_y(m, r, f, low):
        if r in (1, 2):
            cfly[m, 0, 8 * (r - 1) : 8 * r, :] = f[:, 0:128]
            cfly[m, 1, 8 * (r - 1) : 8 * r, :] = low[:, 128:256]

    def coarse_emit(m, r, q, div):
        rows = pl.ds(8 * r, 8)
        cn[m, rows, :] = q - courant * (cx[m, rows, :] + cz[m, rows, :] + div)

    z_pass(cq, cz, 256, 8)
    x_pass(cq, cx, 256, coarse_keep_x)
    y_pass(cq, 256, 8, coarse_emit, coarse_keep_y)
    put_ring(
        mids,
        lambda m, a, b, t: 0.5
        * (cq[m, a:b, 128 * t : 128 * t + 128] + cn[m, a:b, 128 * t : 128 * t + 128]),
    )
    pending += spread(mids, mid_s, mid_r)

    for c in halo[2:]:
        c.start()

    site_v = jnp.full((24, 128), site, jnp.int32)
    row32 = iota((32, 128), 0)
    mine = iota((32, 128), 1) // 8 == row32 // 2

    def ghosts(buf):
        got = jnp.zeros((24, 128), F32)
        for s in range(GY):
            got = jnp.where(site_v == s, buf[s], got)
        wide = dot(got[0:16], spread_x[...])
        lows = jnp.concatenate([jnp.where(mine, got[10 + m : 11 + m], 0.0) for m in range(NV)], axis=0)
        highs = jnp.concatenate([jnp.where(mine, got[15 + m : 16 + m], 0.0) for m in range(NV)], axis=0)
        side = dot(jnp.concatenate([lows, highs], axis=1), spread_y[...])
        edge = iota((8, 512), 0) < 4
        for m in range(NV):
            fq[m, 32:40, 0:512] = jnp.where(edge, wide[5 + m : 6 + m], wide[m : m + 1])
            fq[m, 0:32, 512:640] = side[32 * m : 32 * m + 32]

    def fine_step(first):
        def keep_x(m, lanes, f, low):
            if first:
                xf[m : m + 1, lanes] = f[39:40]
                xf[5 + m : 6 + m, lanes] = f[31:32]
            else:
                xf[m : m + 1, lanes] += f[39:40]
                xf[5 + m : 6 + m, lanes] += f[31:32]

        def keep_y(m, r, f, low):
            at = 64 * m + 8 * r
            if first:
                yf[at : at + 8, :] = f[:, 512:640]
                yf[at + 32 : at + 40, :] = f[:, 384:512]
            else:
                yf[at : at + 8, :] += f[:, 512:640]
                yf[at + 32 : at + 40, :] += f[:, 384:512]

        def emit(m, r, q, div):
            rows = pl.ds(8 * r, 8)
            new = q - courant * (fx[m, rows, :] + fz[m, rows, :] + div)
            if first:
                fq[m, rows, 0:512] = new
            else:
                fine_out[m, rows, :] = new
                for t in range(4):
                    ps[t, 32 * m + 8 * r : 32 * m + 8 * r + 8, :] = new[:, 128 * t : 128 * t + 128]

        x_pass(fq, fx, 512, keep_x)
        y_pass(fq, 512, 16, emit, keep_y)

    load_f.wait()
    z_pass(fq, fz, 512, 16)
    received(ring, ring_s, ring_r)
    ghosts(ring)
    fine_step(True)
    z_pass(fq, fz, 512, 16)
    received(mids, mid_s, mid_r)
    ghosts(mids)
    fine_step(False)
    pairs = jnp.concatenate(
        [ps[t, pl.ds(0, 80, stride=2), :] + ps[t, pl.ds(1, 80, stride=2), :] for t in range(4)], axis=1
    )
    means = dot(jnp.concatenate([pairs, xf[...]], axis=0), gather_x[...])
    for a in range(6):
        pieces[a] = means[16 * a : 16 * a + 16]
    cols = dot(yf[pl.ds(0, 160, stride=2), :] + yf[pl.ds(1, 160, stride=2), :], gather_y[...])
    acc = jnp.zeros((16, 128), F32)
    for n in range(10):
        acc = jnp.where(lane16 // 8 == n, cols[16 * n : 16 * n + 16], acc)
    pieces[6] = acc

    def exchange_one(i, p, s):
        return pltpu.make_async_remote_copy(
            src_ref=pieces.at[p], dst_ref=stage.at[s], send_sem=one_s.at[i], recv_sem=one_r.at[s],
            device_id=(gx, p), device_id_type=MESH,
        )

    def exchange_two(i, p, s):
        return pltpu.make_async_remote_copy(
            src_ref=order.at[p], dst_ref=arrived.at[s], send_sem=two_s.at[i], recv_sem=two_r.at[s],
            device_id=(gx, p), device_id_type=MESH,
        )

    for i, p in enumerate(peers):
        @pl.when(p != GY - 1)
        def _():
            exchange_one(i, p, gy).start()

    stage[gy] = pieces[gy]

    @pl.when(gy != GY - 1)
    def _():
        for i, k in enumerate(far):
            exchange_one(i, gy, lax.rem(gy + GY - k, GY)).wait_recv()
        tags = [jnp.broadcast_to(ring[s, 23:24, :], (16, 128)) for s in range(GY)]
        for d in range(GY):
            acc = jnp.zeros((16, 128), F32)
            for s in range(GY):
                acc = jnp.where(tags[s] == float(d), stage[s], acc)
            order[d] = acc
        for i, p in enumerate(peers):
            exchange_two(i, p, gy).start()
        arrived[gy] = order[gy]

    @pl.when(odd == 0)
    def _():
        pl.semaphore_wait(ready, 2)
        for c in halo[:2]:
            c.start()

    for c in halo:
        c.wait_recv()
    for m in range(NV):
        two = jnp.concatenate([hxr[0, 2 * m : 2 * m + 2, :], jnp.zeros((4, 256), F32), hxr[1, 2 * m : 2 * m + 2, :]], axis=0)
        cq[m, 32:40, 0:256] = two
        for r in range(4):
            n = 4 * m + r
            high = pltpu.roll(hyr[0, n // 8], (-16 * (n % 8)) % 128, 1) if n % 8 else hyr[0, n // 8]
            low = pltpu.roll(hyr[1, n // 8], (112 - 16 * (n % 8)) % 128, 1) if n % 8 != 7 else hyr[1, n // 8]
            cq[m, 8 * r : 8 * r + 8, 256:384] = jnp.where(
                lane8 < 16, high, jnp.where(lane8 >= 112, low, 0.0)
            )
    x_pass(cq, cx, 256, coarse_keep_x)
    y_pass(cq, 256, 8, coarse_emit, coarse_keep_y)

    weight = jnp.full((16, 128), live, jnp.int32).astype(F32) * courant
    w8 = weight[0:8]
    present = jnp.full((16, 128), live, jnp.int32) > 0
    row8 = iota((8, 128), 0)

    for i, k in enumerate(far):
        src = lax.rem(gy + GY - k, GY)

        @pl.when(src != GY - 1)
        def _():
            exchange_two(i, src, src).wait_recv()

    for m in range(NV):
        mean = pltpu.roll(arrived[m], 64, 1)
        left = cn[m, 8:24, 0:128]
        right = cn[m, 8:24, 128:256]
        left = jnp.where(present & (lane16 >= 64), mean, left)
        right = jnp.where(present & (lane16 < 64), mean, right)
        low = pltpu.roll(arrived[6], (56 - 16 * m) % 128, 1)
        high = pltpu.roll(arrived[6], (56 - 16 * m) % 128, 1)
        left = left + jnp.where(lane16 // 8 == 7, weight * (cfly[m, 0] - low), 0.0)
        right = right + jnp.where(lane16 // 8 == 8, weight * (high - cfly[m, 1]), 0.0)
        cn[m, 8:24, 0:128] = left
        cn[m, 8:24, 128:256] = right
        low = jnp.broadcast_to(pltpu.roll(arrived[5, m : m + 1, :], 64, 1), (8, 128))
        high = jnp.broadcast_to(pltpu.roll(arrived[5, 5 + m : 6 + m, :], 64, 1), (8, 128))
        for t in range(2):
            lanes = pl.ds(128 * t, 128)
            inside = lane8 >= 64 if t == 0 else lane8 < 64
            cn[m, 0:8, lanes] += jnp.where(inside & (row8 == 7), w8 * (cflx[m, 0, :, lanes] - low), 0.0)
            cn[m, 24:32, lanes] += jnp.where(inside & (row8 == 0), w8 * (high - cflx[m, 1, :, lanes]), 0.0)

    for c in pending + halo:
        c.wait_send()
    for i, p in enumerate(peers):
        @pl.when(p != GY - 1)
        def _():
            exchange_one(i, p, gy).wait_send()

    @pl.when(gy != GY - 1)
    def _():
        for i, p in enumerate(peers):
            exchange_two(i, p, gy).wait_send()


def shards(coarse_state, fine_state, slot_site, box_live):
    dma = pltpu.SemaphoreType.DMA
    vm = lambda *s: pltpu.VMEM(s, F32)
    coarse_out, fine_out = pl.pallas_call(
        kernel,
        out_shape=(
            pltpu.VMEM((NV, 32, 256), F32),
            pltpu.VMEM((NV, 32, 512), F32),
        ),
        in_specs=[
            pl.BlockSpec(memory_space=pl.ANY),
            pl.BlockSpec(memory_space=pl.ANY),
            pl.BlockSpec(memory_space=pltpu.SMEM),
            pl.BlockSpec(memory_space=pltpu.SMEM),
        ],
        out_specs=[pl.BlockSpec(memory_space=pltpu.VMEM)] * 2,
        scratch_shapes=[
            vm(NV, 40, 384), vm(NV, 40, 640),
            vm(NV, 32, 256), vm(NV, 32, 256),
            vm(NV, 32, 512), vm(NV, 32, 512),
            vm(NV, 2, 8, 256), vm(NV, 2, 16, 128),
            vm(16, 512), vm(320, 128), vm(4, 160, 128),
            vm(128, 512), vm(256, 128), vm(512, 128), vm(128, 128),
            vm(GY, 24, 128), vm(GY, 24, 128),
            vm(GY, 16, 128), vm(GY, 16, 128), vm(GY, 16, 128), vm(GY, 16, 128),
            vm(2, 16, 256), vm(2, 16, 256), vm(2, 3, 8, 128), vm(2, 3, 8, 128),
            dma((2,)),
            dma((7,)), dma((8,)), dma((7,)), dma((8,)), dma((7,)), dma((8,)), dma((7,)), dma((8,)),
            dma((4,)), dma((4,)), pltpu.SemaphoreType.REGULAR,
        ],
        compiler_params=pltpu.CompilerParams(collective_id=0, has_side_effects=True),
        name="amr_step",
    )(coarse_state, fine_state.reshape(NV, 32, 512), slot_site, box_live)
    return coarse_out, fine_out.reshape(1, NV, 32, 512)


def solution(mesh):
    return jax.shard_map(
        shards,
        mesh=mesh,
        in_specs=(
            P(None, "gx", "gy"),
            P(("gx", "gy"), None, None, None),
            P(("gx", "gy"), None),
            P(("gx", "gy")),
        ),
        out_specs=(P(None, "gx", "gy"), P(("gx", "gy"), None, None, None)),
        check_vma=False,
    )
```

```python
import jax
import jax.numpy as jnp
from jax import lax
from jax.experimental import pallas as pl
from jax.experimental.pallas import tpu as pltpu
from jax.sharding import PartitionSpec as P

NV = 5
GY = 8
courant = 0.2
drift = (0.5, 0.3, 0.2)
signal = (1.5, 1.3, 1.2)
MESH = pl.DeviceIdType.MESH
F32 = jnp.float32


def iota(shape, dim):
    return lax.broadcasted_iota(jnp.int32, shape, dim)


def up(x, n, axis):
    return pltpu.roll(x, x.shape[axis] - n, axis)


def down(x, n, axis):
    return pltpu.roll(x, n, axis)


def z_up(x, depth):
    last = iota(x.shape, 1) % depth == depth - 1
    return jnp.where(last, pltpu.roll(x, depth - 1, 1), pltpu.roll(x, 127, 1))


def z_down(x, depth):
    first = iota(x.shape, 1) % depth == 0
    return jnp.where(first, pltpu.roll(x, 129 - depth, 1), pltpu.roll(x, 1, 1))


def minmod(a, b):
    return jnp.maximum(jnp.minimum(a, b), 0.0) + jnp.minimum(jnp.maximum(a, b), 0.0)


def face_fluxes(q, d, ahead, behind):
    plus = 0.5 * (drift[d] + signal[d])
    minus = 0.5 * (drift[d] - signal[d])
    left, right = [], []
    for v in q:
        diff = ahead(v) - v
        half = 0.5 * minmod(behind(diff), diff)
        left.append(v + half)
        right.append(v - half)

    def side(s, coef):
        vn = 0.5 * s[1 + d]
        out = [coef * x for x in s]
        out[0] = out[0] + vn
        out[4] = out[4] + vn
        out[1 + d] = out[1 + d] + 0.5 * s[4]
        return out

    a, b = side(left, plus), side(right, minus)
    return [x + ahead(y) for x, y in zip(a, b)]


def z_pass(q_ref, out_ref, width, depth):
    for t in range(width // 128):
        lanes = pl.ds(128 * t, 128)
        q = [q_ref[m, 0:32, lanes] for m in range(NV)]
        f = face_fluxes(q, 2, lambda x: z_up(x, depth), lambda x: z_down(x, depth))
        for m in range(NV):
            out_ref[m, :, lanes] = f[m] - z_down(f[m], depth)


def x_pass(q_ref, out_ref, width, keep):
    for t in range(width // 128):
        lanes = pl.ds(128 * t, 128)
        q = [q_ref[m, :, lanes] for m in range(NV)]
        f = face_fluxes(q, 0, lambda x: up(x, 1, 0), lambda x: down(x, 1, 0))
        for m in range(NV):
            low = down(f[m], 1, 0)
            out_ref[m, :, lanes] = (f[m] - low)[0:32]
            keep(m, lanes, f[m], low)


def y_pass(q_ref, width, depth, emit, keep):
    for r in range(4):
        rows = pl.ds(8 * r, 8)
        q = [q_ref[m, rows, :] for m in range(NV)]
        f = face_fluxes(q, 1, lambda x: up(x, depth, 1), lambda x: down(x, depth, 1))
        for m in range(NV):
            low = down(f[m], depth, 1)
            keep(m, r, f[m], low)
            emit(m, r, q[m][:, 0:width], (f[m] - low)[:, 0:width])


def dot(a, b):
    return jnp.dot(a, b, precision=lax.Precision.HIGHEST, preferred_element_type=F32)


def kernel(
    coarse, fine, site_hbm, live_ref, cn, fine_out,
    cq, fq, cz, cx, fz, fx, cflx, cfly, xf, yf, ps,
    spread_x, spread_y, gather_x, gather_y, ring, mids, pieces, stage, order, arrived,
    hxs, hxr, hys, hyr, site_ref, tags,
    in_sem, ring_s, ring_r, mid_s, mid_r, one_s, one_r, two_s, two_r, hal_s, hal_r, tag_s, tag_r, ready,
):
    gx, gy = lax.axis_index("gx"), lax.axis_index("gy")
    ngx = lax.axis_size("gx")
    load_c = pltpu.make_async_copy(coarse, cq.at[:, 0:32, 0:256], in_sem.at[0])
    load_f = pltpu.make_async_copy(fine, fq.at[:, 0:32, 0:512], in_sem.at[1])
    load_s = pltpu.make_async_copy(site_hbm, site_ref, in_sem.at[2])
    barrier = pltpu.get_barrier_semaphore()
    gx_lo, gx_hi = lax.rem(gx + ngx - 1, ngx), lax.rem(gx + 1, ngx)
    odd = lax.rem(gx, 2)

    @pl.when(odd == 0)
    def _():
        for g in (gx_lo, gx_hi):
            pl.semaphore_signal(barrier, inc=1, device_id=(g, gy), device_id_type=MESH)

    far = (4, 3, 5, 2, 6, 1, 7)
    peers = [lax.rem(gy + k, GY) for k in far]
    for p in peers:
        pl.semaphore_signal(barrier, inc=1, device_id=(gx, p), device_id_type=MESH)

    load_c.start()
    load_s.start()
    load_f.start()

    k, o = iota((128, 512), 0), iota((128, 512), 1)
    spread_x[...] = jnp.where(k == (o // 32) * 8 + (o % 16) // 2, 1.0, 0.0)
    k, o = iota((256, 128), 0), iota((256, 128), 1)
    hit = (k % 8 == (o % 16) // 2) & (((k < 128) & (o >= 96)) | ((k >= 128) & (o < 32)))
    spread_y[...] = jnp.where(hit, 1.0, 0.0)
    k, o = iota((512, 128), 0), iota((512, 128), 1)
    gather_x[...] = jnp.where(o == (k // 32) * 8 + (k % 16) // 2, 0.125, 0.0)
    k, o = iota((128, 128), 0), iota((128, 128), 1)
    gather_y[...] = jnp.where((k >= 112) & ((k % 16) // 2 == o % 8), 0.125, 0.0)
    pick_low = jnp.where(k == 56 + o % 8, 1.0, 0.0)
    pick_high = jnp.where(k == 64 + o % 8, 1.0, 0.0)

    cq[:, 32:40, :] = jnp.zeros((NV, 8, 384), F32)
    cq[:, 0:32, 256:384] = jnp.zeros((NV, 32, 128), F32)
    fq[:, 32:40, :] = jnp.zeros((NV, 8, 640), F32)
    xf[...] = jnp.zeros((16, 512), F32)

    lane16 = iota((16, 128), 1)
    own = lane16 // 8 == iota((16, 128), 0)

    def put_ring(dst, get):
        for m in range(NV):
            for face, row in ((0, 7), (1, 24)):
                first, second = get(m, row, row + 1, 0), get(m, row, row + 1, 1)
                both = jnp.where(
                    iota((1, 128), 1) < 64, pltpu.roll(first, 64, 1), pltpu.roll(second, 64, 1)
                )
                dst[gy, m, face : face + 1, :] = both
        for face, pick in ((2, pick_low), (3, pick_high)):
            cols = jnp.concatenate([get(m, 8, 24, face - 2) for m in range(NV)], axis=0)
            copies = dot(cols, pick)
            for m in range(NV):
                part = jnp.where(own, copies[16 * m : 16 * m + 16], 0.0)
                dst[gy, m, face : face + 1, :] = jnp.sum(part, axis=0, keepdims=True)

    load_c.wait()
    load_s.wait()
    site = site_ref[0, 0]
    live = live_ref[0]
    tags[gy] = jnp.full((1, 128), site, jnp.int32).astype(F32)
    put_ring(ring, lambda m, a, b, t: cq[m, a:b, 128 * t : 128 * t + 128])
    for m in range(NV):
        hxs[0, 2 * m : 2 * m + 2, :] = cq[m, 0:2, 0:256]
        hxs[1, 2 * m : 2 * m + 2, :] = cq[m, 30:32, 0:256]
    lane8 = iota((8, 128), 1)
    for side, tile, base in ((0, 0, 0), (1, 1, 112)):
        for g in range(3):
            acc = jnp.zeros((8, 128), F32)
            for n in range(8 * g, min(8 * g + 8, 20)):
                block = cq[n // 4, 8 * (n % 4) : 8 * (n % 4) + 8, 128 * tile : 128 * tile + 128]
                moved = pltpu.roll(block, (16 * (n % 8) - base) % 128, 1) if (16 * (n % 8) - base) % 128 else block
                acc = jnp.where(lane8 // 16 == n % 8, moved, acc)
            hys[side, g] = acc

    def spread(buf, sends, recvs):
        out = []
        for i, p in enumerate(peers):
            c = pltpu.make_async_remote_copy(
                src_ref=buf.at[gy], dst_ref=buf.at[gy], send_sem=sends.at[i], recv_sem=recvs.at[gy],
                device_id=(gx, p), device_id_type=MESH,
            )
            c.start()
            out.append(c)
        return out

    def received(buf, sends, recvs):
        for i, k in enumerate(far):
            src = lax.rem(gy + GY - k, GY)
            pltpu.make_async_remote_copy(
                src_ref=buf.at[src], dst_ref=buf.at[src], send_sem=sends.at[i], recv_sem=recvs.at[src],
                device_id=(gx, src), device_id_type=MESH,
            ).wait_recv()

    gy_lo, gy_hi = lax.rem(gy + GY - 1, GY), lax.rem(gy + 1, GY)
    halo = [
        pltpu.make_async_remote_copy(
            src_ref=src, dst_ref=dst, send_sem=hal_s.at[i], recv_sem=hal_r.at[i],
            device_id=where, device_id_type=MESH,
        )
        for i, (src, dst, where) in enumerate(
            (
                (hxs.at[0], hxr.at[0], (gx_lo, gy)),
                (hxs.at[1], hxr.at[1], (gx_hi, gy)),
                (hys.at[0], hyr.at[0], (gx, gy_lo)),
                (hys.at[1], hyr.at[1], (gx, gy_hi)),
            )
        )
    ]
    pl.semaphore_wait(barrier, 7 + 2 * odd)

    @pl.when(odd == 1)
    def _():
        for g in (gx_lo, gx_hi):
            pl.semaphore_signal(ready, inc=1, device_id=(g, gy), device_id_type=MESH)
        for c in halo[:2]:
            c.start()

    pending = spread(ring, ring_s, ring_r)

    def coarse_keep_x(m, lanes, f, low):
        cflx[m, 0, :, lanes] = f[0:8]
        cflx[m, 1, :, lanes] = low[24:32]

    def coarse_keep_y(m, r, f, low):
        if r in (1, 2):
            cfly[m, 0, 8 * (r - 1) : 8 * r, :] = f[:, 0:128]
            cfly[m, 1, 8 * (r - 1) : 8 * r, :] = low[:, 128:256]

    def coarse_emit(m, r, q, div):
        rows = pl.ds(8 * r, 8)
        cn[m, rows, :] = q - courant * (cx[m, rows, :] + cz[m, rows, :] + div)

    z_pass(cq, cz, 256, 8)
    x_pass(cq, cx, 256, coarse_keep_x)
    y_pass(cq, 256, 8, coarse_emit, coarse_keep_y)
    put_ring(
        mids,
        lambda m, a, b, t: 0.5
        * (cq[m, a:b, 128 * t : 128 * t + 128] + cn[m, a:b, 128 * t : 128 * t + 128]),
    )
    pending += spread(mids, mid_s, mid_r)
    pending += spread(tags, tag_s, tag_r)

    for c in halo[2:]:
        c.start()

    site_v = jnp.full((NV, 4, 128), site, jnp.int32)
    row32 = iota((32, 128), 0)
    mine = iota((32, 128), 1) // 8 == row32 // 2

    def ghosts(buf):
        got = jnp.zeros((NV, 4, 128), F32)
        for s in range(GY):
            got = jnp.where(site_v == s, buf[s], got)
        rows = jnp.concatenate([got[m] for m in range(NV)] + [jnp.zeros((4, 128), F32)], axis=0)
        wide = dot(rows, spread_x[...])
        lows = jnp.concatenate([jnp.where(mine, rows[4 * m + 2 : 4 * m + 3], 0.0) for m in range(NV)], axis=0)
        highs = jnp.concatenate([jnp.where(mine, rows[4 * m + 3 : 4 * m + 4], 0.0) for m in range(NV)], axis=0)
        side = dot(jnp.concatenate([lows, highs], axis=1), spread_y[...])
        edge = iota((8, 512), 0) < 4
        for m in range(NV):
            fq[m, 32:40, 0:512] = jnp.where(edge, wide[4 * m + 1 : 4 * m + 2], wide[4 * m : 4 * m + 1])
            fq[m, 0:32, 512:640] = side[32 * m : 32 * m + 32]

    def fine_step(first):
        def keep_x(m, lanes, f, low):
            if first:
                xf[m : m + 1, lanes] = f[39:40]
                xf[5 + m : 6 + m, lanes] = f[31:32]
            else:
                xf[m : m + 1, lanes] += f[39:40]
                xf[5 + m : 6 + m, lanes] += f[31:32]

        def keep_y(m, r, f, low):
            at = 64 * m + 8 * r
            if first:
                yf[at : at + 8, :] = f[:, 512:640]
                yf[at + 32 : at + 40, :] = f[:, 384:512]
            else:
                yf[at : at + 8, :] += f[:, 512:640]
                yf[at + 32 : at + 40, :] += f[:, 384:512]

        def emit(m, r, q, div):
            rows = pl.ds(8 * r, 8)
            new = q - courant * (fx[m, rows, :] + fz[m, rows, :] + div)
            if first:
                fq[m, rows, 0:512] = new
            else:
                fine_out[m, rows, :] = new
                for t in range(4):
                    ps[t, 32 * m + 8 * r : 32 * m + 8 * r + 8, :] = new[:, 128 * t : 128 * t + 128]

        x_pass(fq, fx, 512, keep_x)
        y_pass(fq, 512, 16, emit, keep_y)

    load_f.wait()
    z_pass(fq, fz, 512, 16)
    received(ring, ring_s, ring_r)
    ghosts(ring)
    fine_step(True)
    z_pass(fq, fz, 512, 16)
    received(mids, mid_s, mid_r)
    ghosts(mids)
    fine_step(False)
    pairs = jnp.concatenate(
        [ps[t, pl.ds(0, 80, stride=2), :] + ps[t, pl.ds(1, 80, stride=2), :] for t in range(4)], axis=1
    )
    means = dot(jnp.concatenate([pairs, xf[...]], axis=0), gather_x[...])
    for a in range(6):
        pieces[a] = means[16 * a : 16 * a + 16]
    cols = dot(yf[pl.ds(0, 160, stride=2), :] + yf[pl.ds(1, 160, stride=2), :], gather_y[...])
    acc = jnp.zeros((16, 128), F32)
    for n in range(10):
        acc = jnp.where(lane16 // 8 == n, cols[16 * n : 16 * n + 16], acc)
    pieces[6] = acc

    def exchange_one(i, p, s):
        return pltpu.make_async_remote_copy(
            src_ref=pieces.at[p], dst_ref=stage.at[s], send_sem=one_s.at[i], recv_sem=one_r.at[s],
            device_id=(gx, p), device_id_type=MESH,
        )

    def exchange_two(i, p, s):
        return pltpu.make_async_remote_copy(
            src_ref=order.at[p], dst_ref=arrived.at[s], send_sem=two_s.at[i], recv_sem=two_r.at[s],
            device_id=(gx, p), device_id_type=MESH,
        )

    for i, p in enumerate(peers):
        @pl.when(p != GY - 1)
        def _():
            exchange_one(i, p, gy).start()

    stage[gy] = pieces[gy]

    received(tags, tag_s, tag_r)

    @pl.when(gy != GY - 1)
    def _():
        for i, k in enumerate(far):
            exchange_one(i, gy, lax.rem(gy + GY - k, GY)).wait_recv()
        owner = [jnp.broadcast_to(tags[s], (16, 128)) for s in range(GY)]
        for d in range(GY):
            acc = jnp.zeros((16, 128), F32)
            for s in range(GY):
                acc = jnp.where(owner[s] == float(d), stage[s], acc)
            order[d] = acc
        for i, p in enumerate(peers):
            exchange_two(i, p, gy).start()
        arrived[gy] = order[gy]

    @pl.when(odd == 0)
    def _():
        pl.semaphore_wait(ready, 2)
        for c in halo[:2]:
            c.start()

    for c in halo:
        c.wait_recv()
    for m in range(NV):
        two = jnp.concatenate([hxr[0, 2 * m : 2 * m + 2, :], jnp.zeros((4, 256), F32), hxr[1, 2 * m : 2 * m + 2, :]], axis=0)
        cq[m, 32:40, 0:256] = two
        for r in range(4):
            n = 4 * m + r
            high = pltpu.roll(hyr[0, n // 8], (-16 * (n % 8)) % 128, 1) if n % 8 else hyr[0, n // 8]
            low = pltpu.roll(hyr[1, n // 8], (112 - 16 * (n % 8)) % 128, 1) if n % 8 != 7 else hyr[1, n // 8]
            cq[m, 8 * r : 8 * r + 8, 256:384] = jnp.where(
                lane8 < 16, high, jnp.where(lane8 >= 112, low, 0.0)
            )
    x_pass(cq, cx, 256, coarse_keep_x)
    y_pass(cq, 256, 8, coarse_emit, coarse_keep_y)

    weight = jnp.full((16, 128), live, jnp.int32).astype(F32) * courant
    w8 = weight[0:8]
    present = jnp.full((16, 128), live, jnp.int32) > 0
    row8 = iota((8, 128), 0)

    for i, k in enumerate(far):
        src = lax.rem(gy + GY - k, GY)

        @pl.when(src != GY - 1)
        def _():
            exchange_two(i, src, src).wait_recv()

    for m in range(NV):
        mean = pltpu.roll(arrived[m], 64, 1)
        left = cn[m, 8:24, 0:128]
        right = cn[m, 8:24, 128:256]
        left = jnp.where(present & (lane16 >= 64), mean, left)
        right = jnp.where(present & (lane16 < 64), mean, right)
        low = pltpu.roll(arrived[6], (56 - 16 * m) % 128, 1)
        high = pltpu.roll(arrived[6], (56 - 16 * m) % 128, 1)
        left = left + jnp.where(lane16 // 8 == 7, weight * (cfly[m, 0] - low), 0.0)
        right = right + jnp.where(lane16 // 8 == 8, weight * (high - cfly[m, 1]), 0.0)
        cn[m, 8:24, 0:128] = left
        cn[m, 8:24, 128:256] = right
        low = jnp.broadcast_to(pltpu.roll(arrived[5, m : m + 1, :], 64, 1), (8, 128))
        high = jnp.broadcast_to(pltpu.roll(arrived[5, 5 + m : 6 + m, :], 64, 1), (8, 128))
        for t in range(2):
            lanes = pl.ds(128 * t, 128)
            inside = lane8 >= 64 if t == 0 else lane8 < 64
            cn[m, 0:8, lanes] += jnp.where(inside & (row8 == 7), w8 * (cflx[m, 0, :, lanes] - low), 0.0)
            cn[m, 24:32, lanes] += jnp.where(inside & (row8 == 0), w8 * (high - cflx[m, 1, :, lanes]), 0.0)

    for c in pending + halo:
        c.wait_send()
    for i, p in enumerate(peers):
        @pl.when(p != GY - 1)
        def _():
            exchange_one(i, p, gy).wait_send()

    @pl.when(gy != GY - 1)
    def _():
        for i, p in enumerate(peers):
            exchange_two(i, p, gy).wait_send()


def shards(coarse_state, fine_state, slot_site, box_live):
    dma = pltpu.SemaphoreType.DMA
    vm = lambda *s: pltpu.VMEM(s, F32)
    coarse_out, fine_out = pl.pallas_call(
        kernel,
        out_shape=(
            pltpu.VMEM((NV, 32, 256), F32),
            pltpu.VMEM((NV, 32, 512), F32),
        ),
        in_specs=[
            pl.BlockSpec(memory_space=pl.ANY),
            pl.BlockSpec(memory_space=pl.ANY),
            pl.BlockSpec(memory_space=pl.ANY),
            pl.BlockSpec(memory_space=pltpu.SMEM),
        ],
        out_specs=[pl.BlockSpec(memory_space=pltpu.VMEM)] * 2,
        scratch_shapes=[
            vm(NV, 40, 384), vm(NV, 40, 640),
            vm(NV, 32, 256), vm(NV, 32, 256),
            vm(NV, 32, 512), vm(NV, 32, 512),
            vm(NV, 2, 8, 256), vm(NV, 2, 16, 128),
            vm(16, 512), vm(320, 128), vm(4, 160, 128),
            vm(128, 512), vm(256, 128), vm(512, 128), vm(128, 128),
            vm(GY, NV, 4, 128), vm(GY, NV, 4, 128),
            vm(GY, 16, 128), vm(GY, 16, 128), vm(GY, 16, 128), vm(GY, 16, 128),
            vm(2, 16, 256), vm(2, 16, 256), vm(2, 3, 8, 128), vm(2, 3, 8, 128),
            pltpu.SMEM((1, 2), jnp.int32), vm(GY, 1, 128),
            dma((3,)),
            dma((7,)), dma((8,)), dma((7,)), dma((8,)), dma((7,)), dma((8,)), dma((7,)), dma((8,)),
            dma((4,)), dma((4,)), dma((7,)), dma((8,)), pltpu.SemaphoreType.REGULAR,
        ],
        compiler_params=pltpu.CompilerParams(collective_id=0, has_side_effects=True),
        name="amr_step",
    )(coarse_state, fine_state.reshape(NV, 32, 512), slot_site, box_live)
    return coarse_out, fine_out.reshape(1, NV, 32, 512)


def solution(mesh):
    return jax.shard_map(
        shards,
        mesh=mesh,
        in_specs=(
            P(None, "gx", "gy"),
            P(("gx", "gy"), None, None, None),
            P(("gx", "gy"), None),
            P(("gx", "gy")),
        ),
        out_specs=(P(None, "gx", "gy"), P(("gx", "gy"), None, None, None)),
        check_vma=False,
    )
```

```python
import jax
import jax.numpy as jnp
from jax import lax
from jax.experimental import pallas as pl
from jax.experimental.pallas import tpu as pltpu
from jax.sharding import PartitionSpec as P

NV = 5
GY = 8
courant = 0.2
drift = (0.5, 0.3, 0.2)
signal = (1.5, 1.3, 1.2)
MESH = pl.DeviceIdType.MESH
F32 = jnp.float32
BF16 = jnp.bfloat16


def iota(shape, dim):
    return lax.broadcasted_iota(jnp.int32, shape, dim)


def up(x, n, axis):
    return pltpu.roll(x, x.shape[axis] - n, axis)


def down(x, n, axis):
    return pltpu.roll(x, n, axis)


def z_up(x, depth):
    last = iota(x.shape, 1) % depth == depth - 1
    return jnp.where(last, pltpu.roll(x, depth - 1, 1), pltpu.roll(x, 127, 1))


def z_down(x, depth):
    first = iota(x.shape, 1) % depth == 0
    return jnp.where(first, pltpu.roll(x, 129 - depth, 1), pltpu.roll(x, 1, 1))


def minmod(a, b):
    return jnp.maximum(jnp.minimum(a, b), 0.0) + jnp.minimum(jnp.maximum(a, b), 0.0)


def face_fluxes(q, d, ahead, behind):
    plus = 0.5 * (drift[d] + signal[d])
    minus = 0.5 * (drift[d] - signal[d])
    left, right = [], []
    for v in q:
        diff = ahead(v) - v
        half = 0.5 * minmod(behind(diff), diff)
        left.append(v + half)
        right.append(v - half)

    def side(s, coef):
        vn = 0.5 * s[1 + d]
        out = [coef * x for x in s]
        out[0] = out[0] + vn
        out[4] = out[4] + vn
        out[1 + d] = out[1 + d] + 0.5 * s[4]
        return out

    a, b = side(left, plus), side(right, minus)
    return [x + ahead(y) for x, y in zip(a, b)]


def z_pass(q_ref, out_ref, width, depth):
    for t in range(width // 128):
        lanes = pl.ds(128 * t, 128)
        q = [q_ref[m, 0:32, lanes] for m in range(NV)]
        f = face_fluxes(q, 2, lambda x: z_up(x, depth), lambda x: z_down(x, depth))
        for m in range(NV):
            out_ref[m, :, lanes] = f[m] - z_down(f[m], depth)


def x_pass(q_ref, out_ref, width, keep):
    for t in range(width // 128):
        lanes = pl.ds(128 * t, 128)
        q = [q_ref[m, :, lanes] for m in range(NV)]
        f = face_fluxes(q, 0, lambda x: up(x, 1, 0), lambda x: down(x, 1, 0))
        for m in range(NV):
            low = down(f[m], 1, 0)
            out_ref[m, :, lanes] = (f[m] - low)[0:32]
            keep(m, lanes, f[m], low)


def y_pass(q_ref, width, depth, emit, keep):
    for r in range(4):
        rows = pl.ds(8 * r, 8)
        q = [q_ref[m, rows, :] for m in range(NV)]
        f = face_fluxes(q, 1, lambda x: up(x, depth, 1), lambda x: down(x, depth, 1))
        for m in range(NV):
            low = down(f[m], depth, 1)
            keep(m, r, f[m], low)
            emit(m, r, q[m][:, 0:width], (f[m] - low)[:, 0:width])


def dot(a, b):
    high = a.astype(BF16)
    rest = a - high.astype(F32)
    middle = rest.astype(BF16)
    low = (rest - middle.astype(F32)).astype(BF16)
    parts = [jnp.dot(p, b, preferred_element_type=F32) for p in (high, middle, low)]
    return parts[0] + (parts[1] + parts[2])


def kernel(
    coarse, fine, site_hbm, live_ref, cn, fine_out,
    cq, fq, cz, cx, fz, fx, cflx, cfly, xf, yf, ps,
    spread_x, spread_y, gather_x, gather_y, ring, mids, pieces, stage, order, arrived,
    hxs, hxr, hys, hyr, site_ref, tags,
    in_sem, ring_s, ring_r, mid_s, mid_r, one_s, one_r, two_s, two_r, hal_s, hal_r, tag_s, tag_r, ready,
):
    gx, gy = lax.axis_index("gx"), lax.axis_index("gy")
    ngx = lax.axis_size("gx")
    load_c = pltpu.make_async_copy(coarse, cq.at[:, 0:32, 0:256], in_sem.at[0])
    load_f = pltpu.make_async_copy(fine, fq.at[:, 0:32, 0:512], in_sem.at[1])
    load_s = pltpu.make_async_copy(site_hbm, site_ref, in_sem.at[2])
    barrier = pltpu.get_barrier_semaphore()
    gx_lo, gx_hi = lax.rem(gx + ngx - 1, ngx), lax.rem(gx + 1, ngx)
    odd = lax.rem(gx, 2)

    @pl.when(odd == 0)
    def _():
        for g in (gx_lo, gx_hi):
            pl.semaphore_signal(barrier, inc=1, device_id=(g, gy), device_id_type=MESH)

    far = (4, 3, 5, 2, 6, 1, 7)
    peers = [lax.rem(gy + k, GY) for k in far]
    for p in peers:
        pl.semaphore_signal(barrier, inc=1, device_id=(gx, p), device_id_type=MESH)

    load_c.start()
    load_s.start()
    load_f.start()

    k, o = iota((128, 512), 0), iota((128, 512), 1)
    spread_x[...] = jnp.where(k == (o // 32) * 8 + (o % 16) // 2, 1.0, 0.0).astype(BF16)
    k, o = iota((256, 128), 0), iota((256, 128), 1)
    hit = (k % 8 == (o % 16) // 2) & (((k < 128) & (o >= 96)) | ((k >= 128) & (o < 32)))
    spread_y[...] = jnp.where(hit, 1.0, 0.0).astype(BF16)
    k, o = iota((512, 128), 0), iota((512, 128), 1)
    gather_x[...] = jnp.where(o == (k // 32) * 8 + (k % 16) // 2, 0.125, 0.0).astype(BF16)
    k, o = iota((128, 128), 0), iota((128, 128), 1)
    gather_y[...] = jnp.where((k >= 112) & ((k % 16) // 2 == o % 8), 0.125, 0.0).astype(BF16)
    pick_low = jnp.where(k == 56 + o % 8, 1.0, 0.0).astype(BF16)
    pick_high = jnp.where(k == 64 + o % 8, 1.0, 0.0).astype(BF16)

    cq[:, 32:40, :] = jnp.zeros((NV, 8, 384), F32)
    cq[:, 0:32, 256:384] = jnp.zeros((NV, 32, 128), F32)
    fq[:, 32:40, :] = jnp.zeros((NV, 8, 640), F32)
    xf[...] = jnp.zeros((16, 512), F32)

    lane16 = iota((16, 128), 1)
    own = lane16 // 8 == iota((16, 128), 0)

    def put_ring(dst, get):
        for m in range(NV):
            for face, row in ((0, 7), (1, 24)):
                first, second = get(m, row, row + 1, 0), get(m, row, row + 1, 1)
                both = jnp.where(
                    iota((1, 128), 1) < 64, pltpu.roll(first, 64, 1), pltpu.roll(second, 64, 1)
                )
                dst[gy, m, face : face + 1, :] = both
        for face, pick in ((2, pick_low), (3, pick_high)):
            cols = jnp.concatenate([get(m, 8, 24, face - 2) for m in range(NV)], axis=0)
            copies = dot(cols, pick)
            for m in range(NV):
                part = jnp.where(own, copies[16 * m : 16 * m + 16], 0.0)
                dst[gy, m, face : face + 1, :] = jnp.sum(part, axis=0, keepdims=True)

    load_c.wait()
    load_s.wait()
    site = site_ref[0, 0]
    live = live_ref[0]
    tags[gy] = jnp.full((1, 128), site, jnp.int32).astype(F32)
    put_ring(ring, lambda m, a, b, t: cq[m, a:b, 128 * t : 128 * t + 128])
    for m in range(NV):
        hxs[0, 2 * m : 2 * m + 2, :] = cq[m, 0:2, 0:256]
        hxs[1, 2 * m : 2 * m + 2, :] = cq[m, 30:32, 0:256]
    lane8 = iota((8, 128), 1)
    for side, tile, base in ((0, 0, 0), (1, 1, 112)):
        for g in range(3):
            acc = jnp.zeros((8, 128), F32)
            for n in range(8 * g, min(8 * g + 8, 20)):
                block = cq[n // 4, 8 * (n % 4) : 8 * (n % 4) + 8, 128 * tile : 128 * tile + 128]
                moved = pltpu.roll(block, (16 * (n % 8) - base) % 128, 1) if (16 * (n % 8) - base) % 128 else block
                acc = jnp.where(lane8 // 16 == n % 8, moved, acc)
            hys[side, g] = acc

    def spread(buf, sends, recvs):
        out = []
        for i, p in enumerate(peers):
            c = pltpu.make_async_remote_copy(
                src_ref=buf.at[gy], dst_ref=buf.at[gy], send_sem=sends.at[i], recv_sem=recvs.at[gy],
                device_id=(gx, p), device_id_type=MESH,
            )
            c.start()
            out.append(c)
        return out

    def received(buf, sends, recvs):
        for i, k in enumerate(far):
            src = lax.rem(gy + GY - k, GY)
            pltpu.make_async_remote_copy(
                src_ref=buf.at[src], dst_ref=buf.at[src], send_sem=sends.at[i], recv_sem=recvs.at[src],
                device_id=(gx, src), device_id_type=MESH,
            ).wait_recv()

    gy_lo, gy_hi = lax.rem(gy + GY - 1, GY), lax.rem(gy + 1, GY)
    halo = [
        pltpu.make_async_remote_copy(
            src_ref=src, dst_ref=dst, send_sem=hal_s.at[i], recv_sem=hal_r.at[i],
            device_id=where, device_id_type=MESH,
        )
        for i, (src, dst, where) in enumerate(
            (
                (hxs.at[0], hxr.at[0], (gx_lo, gy)),
                (hxs.at[1], hxr.at[1], (gx_hi, gy)),
                (hys.at[0], hyr.at[0], (gx, gy_lo)),
                (hys.at[1], hyr.at[1], (gx, gy_hi)),
            )
        )
    ]
    pl.semaphore_wait(barrier, 7 + 2 * odd)

    @pl.when(odd == 1)
    def _():
        for g in (gx_lo, gx_hi):
            pl.semaphore_signal(ready, inc=1, device_id=(g, gy), device_id_type=MESH)
        for c in halo[:2]:
            c.start()

    pending = spread(ring, ring_s, ring_r)

    def coarse_keep_x(m, lanes, f, low):
        cflx[m, 0, :, lanes] = f[0:8]
        cflx[m, 1, :, lanes] = low[24:32]

    def coarse_keep_y(m, r, f, low):
        if r in (1, 2):
            cfly[m, 0, 8 * (r - 1) : 8 * r, :] = f[:, 0:128]
            cfly[m, 1, 8 * (r - 1) : 8 * r, :] = low[:, 128:256]

    def coarse_emit(m, r, q, div):
        rows = pl.ds(8 * r, 8)
        cn[m, rows, :] = q - courant * (cx[m, rows, :] + cz[m, rows, :] + div)

    z_pass(cq, cz, 256, 8)
    x_pass(cq, cx, 256, coarse_keep_x)
    y_pass(cq, 256, 8, coarse_emit, coarse_keep_y)
    put_ring(
        mids,
        lambda m, a, b, t: 0.5
        * (cq[m, a:b, 128 * t : 128 * t + 128] + cn[m, a:b, 128 * t : 128 * t + 128]),
    )
    pending += spread(mids, mid_s, mid_r)
    pending += spread(tags, tag_s, tag_r)

    for c in halo[2:]:
        c.start()

    site_v = jnp.full((NV, 4, 128), site, jnp.int32)
    row32 = iota((32, 128), 0)
    mine = iota((32, 128), 1) // 8 == row32 // 2

    def ghosts(buf):
        got = jnp.zeros((NV, 4, 128), F32)
        for s in range(GY):
            got = jnp.where(site_v == s, buf[s], got)
        rows = jnp.concatenate([got[m] for m in range(NV)] + [jnp.zeros((4, 128), F32)], axis=0)
        wide = dot(rows, spread_x[...])
        lows = jnp.concatenate([jnp.where(mine, rows[4 * m + 2 : 4 * m + 3], 0.0) for m in range(NV)], axis=0)
        highs = jnp.concatenate([jnp.where(mine, rows[4 * m + 3 : 4 * m + 4], 0.0) for m in range(NV)], axis=0)
        side = dot(jnp.concatenate([lows, highs], axis=1), spread_y[...])
        edge = iota((8, 512), 0) < 4
        for m in range(NV):
            fq[m, 32:40, 0:512] = jnp.where(edge, wide[4 * m + 1 : 4 * m + 2], wide[4 * m : 4 * m + 1])
            fq[m, 0:32, 512:640] = side[32 * m : 32 * m + 32]

    def fine_step(first):
        def keep_x(m, lanes, f, low):
            if first:
                xf[m : m + 1, lanes] = f[39:40]
                xf[5 + m : 6 + m, lanes] = f[31:32]
            else:
                xf[m : m + 1, lanes] += f[39:40]
                xf[5 + m : 6 + m, lanes] += f[31:32]

        def keep_y(m, r, f, low):
            at = 64 * m + 8 * r
            if first:
                yf[at : at + 8, :] = f[:, 512:640]
                yf[at + 32 : at + 40, :] = f[:, 384:512]
            else:
                yf[at : at + 8, :] += f[:, 512:640]
                yf[at + 32 : at + 40, :] += f[:, 384:512]

        def emit(m, r, q, div):
            rows = pl.ds(8 * r, 8)
            new = q - courant * (fx[m, rows, :] + fz[m, rows, :] + div)
            if first:
                fq[m, rows, 0:512] = new
            else:
                fine_out[m, rows, :] = new
                for t in range(4):
                    ps[t, 32 * m + 8 * r : 32 * m + 8 * r + 8, :] = new[:, 128 * t : 128 * t + 128]

        x_pass(fq, fx, 512, keep_x)
        y_pass(fq, 512, 16, emit, keep_y)

    load_f.wait()
    z_pass(fq, fz, 512, 16)
    received(ring, ring_s, ring_r)
    ghosts(ring)
    fine_step(True)
    z_pass(fq, fz, 512, 16)
    received(mids, mid_s, mid_r)
    ghosts(mids)
    fine_step(False)
    pairs = jnp.concatenate(
        [ps[t, pl.ds(0, 80, stride=2), :] + ps[t, pl.ds(1, 80, stride=2), :] for t in range(4)], axis=1
    )
    means = dot(jnp.concatenate([pairs, xf[...]], axis=0), gather_x[...])
    for a in range(6):
        pieces[a] = means[16 * a : 16 * a + 16]
    cols = dot(yf[pl.ds(0, 160, stride=2), :] + yf[pl.ds(1, 160, stride=2), :], gather_y[...])
    acc = jnp.zeros((16, 128), F32)
    for n in range(10):
        acc = jnp.where(lane16 // 8 == n, cols[16 * n : 16 * n + 16], acc)
    pieces[6] = acc

    def exchange_one(i, p, s):
        return pltpu.make_async_remote_copy(
            src_ref=pieces.at[p], dst_ref=stage.at[s], send_sem=one_s.at[i], recv_sem=one_r.at[s],
            device_id=(gx, p), device_id_type=MESH,
        )

    def exchange_two(i, p, s):
        return pltpu.make_async_remote_copy(
            src_ref=order.at[p], dst_ref=arrived.at[s], send_sem=two_s.at[i], recv_sem=two_r.at[s],
            device_id=(gx, p), device_id_type=MESH,
        )

    for i, p in enumerate(peers):
        @pl.when(p != GY - 1)
        def _():
            exchange_one(i, p, gy).start()

    stage[gy] = pieces[gy]

    received(tags, tag_s, tag_r)

    @pl.when(gy != GY - 1)
    def _():
        for i, k in enumerate(far):
            exchange_one(i, gy, lax.rem(gy + GY - k, GY)).wait_recv()
        owner = [jnp.broadcast_to(tags[s], (16, 128)) for s in range(GY)]
        for d in range(GY):
            acc = jnp.zeros((16, 128), F32)
            for s in range(GY):
                acc = jnp.where(owner[s] == float(d), stage[s], acc)
            order[d] = acc
        for i, p in enumerate(peers):
            exchange_two(i, p, gy).start()
        arrived[gy] = order[gy]

    @pl.when(odd == 0)
    def _():
        pl.semaphore_wait(ready, 2)
        for c in halo[:2]:
            c.start()

    for c in halo:
        c.wait_recv()
    for m in range(NV):
        two = jnp.concatenate([hxr[0, 2 * m : 2 * m + 2, :], jnp.zeros((4, 256), F32), hxr[1, 2 * m : 2 * m + 2, :]], axis=0)
        cq[m, 32:40, 0:256] = two
        for r in range(4):
            n = 4 * m + r
            high = pltpu.roll(hyr[0, n // 8], (-16 * (n % 8)) % 128, 1) if n % 8 else hyr[0, n // 8]
            low = pltpu.roll(hyr[1, n // 8], (112 - 16 * (n % 8)) % 128, 1) if n % 8 != 7 else hyr[1, n // 8]
            cq[m, 8 * r : 8 * r + 8, 256:384] = jnp.where(
                lane8 < 16, high, jnp.where(lane8 >= 112, low, 0.0)
            )
    x_pass(cq, cx, 256, coarse_keep_x)
    y_pass(cq, 256, 8, coarse_emit, coarse_keep_y)

    weight = jnp.full((16, 128), live, jnp.int32).astype(F32) * courant
    w8 = weight[0:8]
    present = jnp.full((16, 128), live, jnp.int32) > 0
    row8 = iota((8, 128), 0)

    for i, k in enumerate(far):
        src = lax.rem(gy + GY - k, GY)

        @pl.when(src != GY - 1)
        def _():
            exchange_two(i, src, src).wait_recv()

    for m in range(NV):
        mean = pltpu.roll(arrived[m], 64, 1)
        left = cn[m, 8:24, 0:128]
        right = cn[m, 8:24, 128:256]
        left = jnp.where(present & (lane16 >= 64), mean, left)
        right = jnp.where(present & (lane16 < 64), mean, right)
        low = pltpu.roll(arrived[6], (56 - 16 * m) % 128, 1)
        high = pltpu.roll(arrived[6], (56 - 16 * m) % 128, 1)
        left = left + jnp.where(lane16 // 8 == 7, weight * (cfly[m, 0] - low), 0.0)
        right = right + jnp.where(lane16 // 8 == 8, weight * (high - cfly[m, 1]), 0.0)
        cn[m, 8:24, 0:128] = left
        cn[m, 8:24, 128:256] = right
        low = jnp.broadcast_to(pltpu.roll(arrived[5, m : m + 1, :], 64, 1), (8, 128))
        high = jnp.broadcast_to(pltpu.roll(arrived[5, 5 + m : 6 + m, :], 64, 1), (8, 128))
        for t in range(2):
            lanes = pl.ds(128 * t, 128)
            inside = lane8 >= 64 if t == 0 else lane8 < 64
            cn[m, 0:8, lanes] += jnp.where(inside & (row8 == 7), w8 * (cflx[m, 0, :, lanes] - low), 0.0)
            cn[m, 24:32, lanes] += jnp.where(inside & (row8 == 0), w8 * (high - cflx[m, 1, :, lanes]), 0.0)

    for c in pending + halo:
        c.wait_send()
    for i, p in enumerate(peers):
        @pl.when(p != GY - 1)
        def _():
            exchange_one(i, p, gy).wait_send()

    @pl.when(gy != GY - 1)
    def _():
        for i, p in enumerate(peers):
            exchange_two(i, p, gy).wait_send()


def shards(coarse_state, fine_state, slot_site, box_live):
    dma = pltpu.SemaphoreType.DMA
    vm = lambda *s: pltpu.VMEM(s, F32)
    coarse_out, fine_out = pl.pallas_call(
        kernel,
        out_shape=(
            pltpu.VMEM((NV, 32, 256), F32),
            pltpu.VMEM((NV, 32, 512), F32),
        ),
        in_specs=[
            pl.BlockSpec(memory_space=pl.ANY),
            pl.BlockSpec(memory_space=pl.ANY),
            pl.BlockSpec(memory_space=pl.ANY),
            pl.BlockSpec(memory_space=pltpu.SMEM),
        ],
        out_specs=[pl.BlockSpec(memory_space=pltpu.VMEM)] * 2,
        scratch_shapes=[
            vm(NV, 40, 384), vm(NV, 40, 640),
            vm(NV, 32, 256), vm(NV, 32, 256),
            vm(NV, 32, 512), vm(NV, 32, 512),
            vm(NV, 2, 8, 256), vm(NV, 2, 16, 128),
            vm(16, 512), vm(320, 128), vm(4, 160, 128),
            *[pltpu.VMEM(s, BF16) for s in ((128, 512), (256, 128), (512, 128), (128, 128))],
            vm(GY, NV, 4, 128), vm(GY, NV, 4, 128),
            vm(GY, 16, 128), vm(GY, 16, 128), vm(GY, 16, 128), vm(GY, 16, 128),
            vm(2, 16, 256), vm(2, 16, 256), vm(2, 3, 8, 128), vm(2, 3, 8, 128),
            pltpu.SMEM((1, 2), jnp.int32), vm(GY, 1, 128),
            dma((3,)),
            dma((7,)), dma((8,)), dma((7,)), dma((8,)), dma((7,)), dma((8,)), dma((7,)), dma((8,)),
            dma((4,)), dma((4,)), dma((7,)), dma((8,)), pltpu.SemaphoreType.REGULAR,
        ],
        compiler_params=pltpu.CompilerParams(collective_id=0, has_side_effects=True),
        name="amr_step",
    )(coarse_state, fine_state.reshape(NV, 32, 512), slot_site, box_live)
    return coarse_out, fine_out.reshape(1, NV, 32, 512)


def solution(mesh):
    return jax.shard_map(
        shards,
        mesh=mesh,
        in_specs=(
            P(None, "gx", "gy"),
            P(("gx", "gy"), None, None, None),
            P(("gx", "gy"), None),
            P(("gx", "gy")),
        ),
        out_specs=(P(None, "gx", "gy"), P(("gx", "gy"), None, None, None)),
        check_vma=False,
    )
```

```python
import jax
import jax.numpy as jnp
from jax import lax
from jax.experimental import pallas as pl
from jax.experimental.pallas import tpu as pltpu
from jax.sharding import PartitionSpec as P

NV = 5
GY = 8
courant = 0.2
drift = (0.5, 0.3, 0.2)
signal = (1.5, 1.3, 1.2)
MESH = pl.DeviceIdType.MESH
F32 = jnp.float32
BF16 = jnp.bfloat16


def iota(shape, dim):
    return lax.broadcasted_iota(jnp.int32, shape, dim)


def up(x, n, axis):
    return pltpu.roll(x, x.shape[axis] - n, axis)


def down(x, n, axis):
    return pltpu.roll(x, n, axis)


def z_up(x, depth):
    last = iota(x.shape, 1) % depth == depth - 1
    return jnp.where(last, pltpu.roll(x, depth - 1, 1), pltpu.roll(x, 127, 1))


def z_down(x, depth):
    first = iota(x.shape, 1) % depth == 0
    return jnp.where(first, pltpu.roll(x, 129 - depth, 1), pltpu.roll(x, 1, 1))


def minmod(a, b):
    return jnp.maximum(jnp.minimum(a, b), 0.0) + jnp.minimum(jnp.maximum(a, b), 0.0)


def face_fluxes(q, d, ahead, behind):
    plus = 0.5 * (drift[d] + signal[d])
    minus = 0.5 * (drift[d] - signal[d])
    left, right = [], []
    for v in q:
        diff = ahead(v) - v
        half = 0.5 * minmod(behind(diff), diff)
        left.append(v + half)
        right.append(v - half)

    def side(s, coef):
        vn = 0.5 * s[1 + d]
        out = [coef * x for x in s]
        out[0] = out[0] + vn
        out[4] = out[4] + vn
        out[1 + d] = out[1 + d] + 0.5 * s[4]
        return out

    a, b = side(left, plus), side(right, minus)
    return [x + ahead(y) for x, y in zip(a, b)]


def z_pass(q_ref, out_ref, width, depth):
    for t in range(width // 128):
        lanes = pl.ds(128 * t, 128)
        q = [q_ref[m, 0:32, lanes] for m in range(NV)]
        f = face_fluxes(q, 2, lambda x: z_up(x, depth), lambda x: z_down(x, depth))
        for m in range(NV):
            out_ref[m, :, lanes] = f[m] - z_down(f[m], depth)


def x_pass(q_ref, out_ref, width, keep):
    for t in range(width // 128):
        lanes = pl.ds(128 * t, 128)
        q = [q_ref[m, :, lanes] for m in range(NV)]
        f = face_fluxes(q, 0, lambda x: up(x, 1, 0), lambda x: down(x, 1, 0))
        for m in range(NV):
            low = down(f[m], 1, 0)
            out_ref[m, :, lanes] = (f[m] - low)[0:32]
            keep(m, lanes, f[m], low)


def y_pass(q_ref, width, depth, emit, keep):
    for r in range(4):
        rows = pl.ds(8 * r, 8)
        q = [q_ref[m, rows, :] for m in range(NV)]
        f = face_fluxes(q, 1, lambda x: up(x, depth, 1), lambda x: down(x, depth, 1))
        for m in range(NV):
            low = down(f[m], depth, 1)
            keep(m, r, f[m], low)
            emit(m, r, q[m][:, 0:width], (f[m] - low)[:, 0:width])


def dot(a, b):
    high = a.astype(BF16)
    rest = a - high.astype(F32)
    middle = rest.astype(BF16)
    low = (rest - middle.astype(F32)).astype(BF16)
    parts = [jnp.dot(p, b, preferred_element_type=F32) for p in (high, middle, low)]
    return parts[0] + (parts[1] + parts[2])


def kernel(
    coarse, fine, site_hbm, live_ref, cn, fine_out,
    cq, fq, cz, cx, fz, fx, cflx, cfly, xf, yf, ps,
    spread_x, spread_y, gather_x, gather_y, ring, mids, pieces, stage, order, arrived,
    hxs, hxr, hys, hyr, site_ref, tags,
    in_sem, ring_s, ring_r, mid_s, mid_r, one_s, one_r, two_s, two_r, hal_s, hal_r, tag_s, tag_r, ready,
):
    gx, gy = lax.axis_index("gx"), lax.axis_index("gy")
    ngx = lax.axis_size("gx")
    load_c = pltpu.make_async_copy(coarse, cq.at[:, 0:32, 0:256], in_sem.at[0])
    load_f = pltpu.make_async_copy(fine, fq.at[:, 0:32, 0:512], in_sem.at[1])
    load_s = pltpu.make_async_copy(site_hbm, site_ref, in_sem.at[2])
    barrier = pltpu.get_barrier_semaphore()
    gx_lo, gx_hi = lax.rem(gx + ngx - 1, ngx), lax.rem(gx + 1, ngx)
    odd = lax.rem(gx, 2)

    @pl.when(odd == 0)
    def _():
        for g in (gx_lo, gx_hi):
            pl.semaphore_signal(barrier, inc=1, device_id=(g, gy), device_id_type=MESH)

    far = (4, 3, 5, 2, 6, 1, 7)
    peers = [lax.rem(gy + k, GY) for k in far]
    for p in peers:
        pl.semaphore_signal(barrier, inc=1, device_id=(gx, p), device_id_type=MESH)

    load_c.start()
    load_s.start()
    load_f.start()

    k, o = iota((128, 512), 0), iota((128, 512), 1)
    spread_x[...] = jnp.where(k == (o // 32) * 8 + (o % 16) // 2, 1.0, 0.0).astype(BF16)
    k, o = iota((256, 128), 0), iota((256, 128), 1)
    hit = (k % 8 == (o % 16) // 2) & (((k < 128) & (o >= 96)) | ((k >= 128) & (o < 32)))
    spread_y[...] = jnp.where(hit, 1.0, 0.0).astype(BF16)
    k, o = iota((512, 128), 0), iota((512, 128), 1)
    gather_x[...] = jnp.where(o == (k // 32) * 8 + (k % 16) // 2, 0.125, 0.0).astype(BF16)
    k, o = iota((128, 128), 0), iota((128, 128), 1)
    gather_y[...] = jnp.where((k >= 112) & ((k % 16) // 2 == o % 8), 0.125, 0.0).astype(BF16)
    pick_low = jnp.where(k == 56 + o % 8, 1.0, 0.0).astype(BF16)
    pick_high = jnp.where(k == 64 + o % 8, 1.0, 0.0).astype(BF16)

    cq[:, 32:40, :] = jnp.zeros((NV, 8, 384), F32)
    cq[:, 0:32, 256:384] = jnp.zeros((NV, 32, 128), F32)
    fq[:, 32:40, :] = jnp.zeros((NV, 8, 640), F32)
    xf[...] = jnp.zeros((16, 512), F32)

    lane16 = iota((16, 128), 1)
    own = lane16 // 8 == iota((16, 128), 0)

    def put_ring(dst, get):
        for m in range(NV):
            for face, row in ((0, 7), (1, 24)):
                first, second = get(m, row, row + 1, 0), get(m, row, row + 1, 1)
                both = jnp.where(
                    iota((1, 128), 1) < 64, pltpu.roll(first, 64, 1), pltpu.roll(second, 64, 1)
                )
                dst[gy, m, face : face + 1, :] = both
        for face, pick in ((2, pick_low), (3, pick_high)):
            cols = jnp.concatenate([get(m, 8, 24, face - 2) for m in range(NV)], axis=0)
            copies = dot(cols, pick)
            for m in range(NV):
                part = jnp.where(own, copies[16 * m : 16 * m + 16], 0.0)
                dst[gy, m, face : face + 1, :] = jnp.sum(part, axis=0, keepdims=True)

    load_c.wait()
    load_s.wait()
    site = site_ref[0, 0]
    live = live_ref[0]
    tags[gy] = jnp.full((1, 128), site, jnp.int32).astype(F32)
    put_ring(ring, lambda m, a, b, t: cq[m, a:b, 128 * t : 128 * t + 128])
    for m in range(NV):
        hxs[0, 2 * m : 2 * m + 2, :] = cq[m, 0:2, 0:256]
        hxs[1, 2 * m : 2 * m + 2, :] = cq[m, 30:32, 0:256]
    lane8 = iota((8, 128), 1)
    for side, tile, base in ((0, 0, 0), (1, 1, 112)):
        for g in range(3):
            acc = jnp.zeros((8, 128), F32)
            for n in range(8 * g, min(8 * g + 8, 20)):
                block = cq[n // 4, 8 * (n % 4) : 8 * (n % 4) + 8, 128 * tile : 128 * tile + 128]
                moved = pltpu.roll(block, (16 * (n % 8) - base) % 128, 1) if (16 * (n % 8) - base) % 128 else block
                acc = jnp.where(lane8 // 16 == n % 8, moved, acc)
            hys[side, g] = acc

    def spread(buf, sends, recvs):
        out = []
        for i, p in enumerate(peers):
            c = pltpu.make_async_remote_copy(
                src_ref=buf.at[gy], dst_ref=buf.at[gy], send_sem=sends.at[i], recv_sem=recvs.at[gy],
                device_id=(gx, p), device_id_type=MESH,
            )
            c.start()
            out.append(c)
        return out

    def received(buf, sends, recvs):
        for i, k in enumerate(far):
            src = lax.rem(gy + GY - k, GY)
            pltpu.make_async_remote_copy(
                src_ref=buf.at[src], dst_ref=buf.at[src], send_sem=sends.at[i], recv_sem=recvs.at[src],
                device_id=(gx, src), device_id_type=MESH,
            ).wait_recv()

    gy_lo, gy_hi = lax.rem(gy + GY - 1, GY), lax.rem(gy + 1, GY)
    halo = [
        pltpu.make_async_remote_copy(
            src_ref=src, dst_ref=dst, send_sem=hal_s.at[i], recv_sem=hal_r.at[i],
            device_id=where, device_id_type=MESH,
        )
        for i, (src, dst, where) in enumerate(
            (
                (hxs.at[0], hxr.at[0], (gx_lo, gy)),
                (hxs.at[1], hxr.at[1], (gx_hi, gy)),
                (hys.at[0], hyr.at[0], (gx, gy_lo)),
                (hys.at[1], hyr.at[1], (gx, gy_hi)),
            )
        )
    ]
    pl.semaphore_wait(barrier, 7 + 2 * odd)

    @pl.when(odd == 1)
    def _():
        for g in (gx_lo, gx_hi):
            pl.semaphore_signal(ready, inc=1, device_id=(g, gy), device_id_type=MESH)
        for c in halo[:2]:
            c.start()

    pending = spread(ring, ring_s, ring_r)

    def coarse_keep_x(m, lanes, f, low):
        cflx[m, 0, :, lanes] = f[0:8]
        cflx[m, 1, :, lanes] = low[24:32]

    def coarse_keep_y(m, r, f, low):
        if r in (1, 2):
            cfly[m, 0, 8 * (r - 1) : 8 * r, :] = f[:, 0:128]
            cfly[m, 1, 8 * (r - 1) : 8 * r, :] = low[:, 128:256]

    def coarse_emit(m, r, q, div):
        rows = pl.ds(8 * r, 8)
        cn[m, rows, :] = q - courant * (cx[m, rows, :] + cz[m, rows, :] + div)

    z_pass(cq, cz, 256, 8)
    x_pass(cq, cx, 256, coarse_keep_x)
    y_pass(cq, 256, 8, coarse_emit, coarse_keep_y)
    put_ring(
        mids,
        lambda m, a, b, t: 0.5
        * (cq[m, a:b, 128 * t : 128 * t + 128] + cn[m, a:b, 128 * t : 128 * t + 128]),
    )
    pending += spread(mids, mid_s, mid_r)
    pending += spread(tags, tag_s, tag_r)

    for c in halo[2:]:
        c.start()

    site_v = jnp.full((NV, 4, 128), site, jnp.int32)
    row32 = iota((32, 128), 0)
    mine = iota((32, 128), 1) // 8 == row32 // 2

    def ghosts(buf):
        got = jnp.zeros((NV, 4, 128), F32)
        for s in range(GY):
            got = jnp.where(site_v == s, buf[s], got)
        rows = jnp.concatenate([got[m] for m in range(NV)] + [jnp.zeros((4, 128), F32)], axis=0)
        wide = dot(rows, spread_x[...])
        lows = jnp.concatenate([jnp.where(mine, rows[4 * m + 2 : 4 * m + 3], 0.0) for m in range(NV)], axis=0)
        highs = jnp.concatenate([jnp.where(mine, rows[4 * m + 3 : 4 * m + 4], 0.0) for m in range(NV)], axis=0)
        side = dot(jnp.concatenate([lows, highs], axis=1), spread_y[...])
        edge = iota((8, 512), 0) < 4
        for m in range(NV):
            fq[m, 32:40, 0:512] = jnp.where(edge, wide[4 * m + 1 : 4 * m + 2], wide[4 * m : 4 * m + 1])
            fq[m, 0:32, 512:640] = side[32 * m : 32 * m + 32]

    def fine_step(first):
        def keep_x(m, lanes, f, low):
            if first:
                xf[m : m + 1, lanes] = f[39:40]
                xf[5 + m : 6 + m, lanes] = f[31:32]
            else:
                xf[m : m + 1, lanes] += f[39:40]
                xf[5 + m : 6 + m, lanes] += f[31:32]

        def keep_y(m, r, f, low):
            at = 64 * m + 8 * r
            if first:
                yf[at : at + 8, :] = f[:, 512:640]
                yf[at + 32 : at + 40, :] = f[:, 384:512]
            else:
                yf[at : at + 8, :] += f[:, 512:640]
                yf[at + 32 : at + 40, :] += f[:, 384:512]

        def emit(m, r, q, div):
            rows = pl.ds(8 * r, 8)
            new = q - courant * (fx[m, rows, :] + fz[m, rows, :] + div)
            if first:
                fq[m, rows, 0:512] = new
            else:
                fine_out[m, rows, :] = new
                for t in range(4):
                    ps[t, 32 * m + 8 * r : 32 * m + 8 * r + 8, :] = new[:, 128 * t : 128 * t + 128]

        x_pass(fq, fx, 512, keep_x)
        y_pass(fq, 512, 16, emit, keep_y)

    load_f.wait()
    z_pass(fq, fz, 512, 16)
    received(ring, ring_s, ring_r)
    ghosts(ring)
    fine_step(True)
    z_pass(fq, fz, 512, 16)
    received(mids, mid_s, mid_r)
    ghosts(mids)
    fine_step(False)
    pairs = jnp.concatenate(
        [ps[t, pl.ds(0, 80, stride=2), :] + ps[t, pl.ds(1, 80, stride=2), :] for t in range(4)], axis=1
    )
    means = dot(jnp.concatenate([pairs, xf[...]], axis=0), gather_x[...])
    for a in range(6):
        pieces[a] = means[16 * a : 16 * a + 16]
    cols = dot(yf[pl.ds(0, 160, stride=2), :] + yf[pl.ds(1, 160, stride=2), :], gather_y[...])
    acc = jnp.zeros((16, 128), F32)
    for n in range(10):
        acc = jnp.where(lane16 // 8 == n, cols[16 * n : 16 * n + 16], acc)
    pieces[6] = acc

    def exchange_one(i, p, s):
        return pltpu.make_async_remote_copy(
            src_ref=pieces.at[p], dst_ref=stage.at[s], send_sem=one_s.at[i], recv_sem=one_r.at[s],
            device_id=(gx, p), device_id_type=MESH,
        )

    def exchange_two(i, p, s):
        return pltpu.make_async_remote_copy(
            src_ref=order.at[p], dst_ref=arrived.at[s], send_sem=two_s.at[i], recv_sem=two_r.at[s],
            device_id=(gx, p), device_id_type=MESH,
        )

    for i, p in enumerate(peers):
        @pl.when(p != GY - 1)
        def _():
            exchange_one(i, p, gy).start()

    stage[gy] = pieces[gy]

    received(tags, tag_s, tag_r)

    @pl.when(gy != GY - 1)
    def _():
        for i, k in enumerate(far):
            exchange_one(i, gy, lax.rem(gy + GY - k, GY)).wait_recv()
        owner = [jnp.broadcast_to(tags[s], (16, 128)) for s in range(GY)]
        for d in range(GY):
            acc = jnp.zeros((16, 128), F32)
            for s in range(GY):
                acc = jnp.where(owner[s] == float(d), stage[s], acc)
            order[d] = acc
        for i, p in enumerate(peers):
            exchange_two(i, p, gy).start()
        arrived[gy] = order[gy]

    @pl.when(odd == 0)
    def _():
        pl.semaphore_wait(ready, 2)
        for c in halo[:2]:
            c.start()

    for c in halo:
        c.wait_recv()
    for m in range(NV):
        two = jnp.concatenate([hxr[0, 2 * m : 2 * m + 2, :], jnp.zeros((4, 256), F32), hxr[1, 2 * m : 2 * m + 2, :]], axis=0)
        cq[m, 32:40, 0:256] = two
        for r in range(4):
            n = 4 * m + r
            high = pltpu.roll(hyr[0, n // 8], (-16 * (n % 8)) % 128, 1) if n % 8 else hyr[0, n // 8]
            low = pltpu.roll(hyr[1, n // 8], (112 - 16 * (n % 8)) % 128, 1) if n % 8 != 7 else hyr[1, n // 8]
            cq[m, 8 * r : 8 * r + 8, 256:384] = jnp.where(
                lane8 < 16, high, jnp.where(lane8 >= 112, low, 0.0)
            )
    x_pass(cq, cx, 256, coarse_keep_x)
    y_pass(cq, 256, 8, coarse_emit, coarse_keep_y)

    weight = jnp.full((16, 128), live, jnp.int32).astype(F32) * courant
    w8 = weight[0:8]
    present = jnp.full((16, 128), live, jnp.int32) > 0
    row8 = iota((8, 128), 0)

    for i, k in enumerate(far):
        src = lax.rem(gy + GY - k, GY)

        @pl.when(src != GY - 1)
        def _():
            exchange_two(i, src, src).wait_recv()

    for m in range(NV):
        mean = pltpu.roll(arrived[m], 64, 1)
        left = cn[m, 8:24, 0:128]
        right = cn[m, 8:24, 128:256]
        left = jnp.where(present & (lane16 >= 64), mean, left)
        right = jnp.where(present & (lane16 < 64), mean, right)
        low = pltpu.roll(arrived[6], (56 - 16 * m) % 128, 1)
        high = pltpu.roll(arrived[6], (56 - 16 * m) % 128, 1)
        left = left + jnp.where(lane16 // 8 == 7, weight * (cfly[m, 0] - low), 0.0)
        right = right + jnp.where(lane16 // 8 == 8, weight * (high - cfly[m, 1]), 0.0)
        cn[m, 8:24, 0:128] = left
        cn[m, 8:24, 128:256] = right
        low = jnp.broadcast_to(pltpu.roll(arrived[5, m : m + 1, :], 64, 1), (8, 128))
        high = jnp.broadcast_to(pltpu.roll(arrived[5, 5 + m : 6 + m, :], 64, 1), (8, 128))
        for t in range(2):
            lanes = pl.ds(128 * t, 128)
            inside = lane8 >= 64 if t == 0 else lane8 < 64
            cn[m, 0:8, lanes] += jnp.where(inside & (row8 == 7), w8 * (cflx[m, 0, :, lanes] - low), 0.0)
            cn[m, 24:32, lanes] += jnp.where(inside & (row8 == 0), w8 * (high - cflx[m, 1, :, lanes]), 0.0)

    for c in pending + halo:
        c.wait_send()
    for i, p in enumerate(peers):
        @pl.when(p != GY - 1)
        def _():
            exchange_one(i, p, gy).wait_send()

    @pl.when(gy != GY - 1)
    def _():
        for i, p in enumerate(peers):
            exchange_two(i, p, gy).wait_send()


def write_out(coarse, fine, coarse_out, fine_out, sem):
    copies = [
        pltpu.make_async_copy(coarse, coarse_out, sem.at[0]),
        pltpu.make_async_copy(fine, fine_out, sem.at[1]),
    ]
    for c in copies:
        c.start()
    for c in copies:
        c.wait()


def shards(coarse_state, fine_state, slot_site, box_live):
    dma = pltpu.SemaphoreType.DMA
    vm = lambda *s: pltpu.VMEM(s, F32)
    coarse_out, fine_out = pl.pallas_call(
        kernel,
        out_shape=(
            pltpu.VMEM((NV, 32, 256), F32),
            pltpu.VMEM((NV, 32, 512), F32),
        ),
        in_specs=[
            pl.BlockSpec(memory_space=pl.ANY),
            pl.BlockSpec(memory_space=pl.ANY),
            pl.BlockSpec(memory_space=pl.ANY),
            pl.BlockSpec(memory_space=pltpu.SMEM),
        ],
        out_specs=[pl.BlockSpec(memory_space=pltpu.VMEM)] * 2,
        scratch_shapes=[
            vm(NV, 40, 384), vm(NV, 40, 640),
            vm(NV, 32, 256), vm(NV, 32, 256),
            vm(NV, 32, 512), vm(NV, 32, 512),
            vm(NV, 2, 8, 256), vm(NV, 2, 16, 128),
            vm(16, 512), vm(320, 128), vm(4, 160, 128),
            *[pltpu.VMEM(s, BF16) for s in ((128, 512), (256, 128), (512, 128), (128, 128))],
            vm(GY, NV, 4, 128), vm(GY, NV, 4, 128),
            vm(GY, 16, 128), vm(GY, 16, 128), vm(GY, 16, 128), vm(GY, 16, 128),
            vm(2, 16, 256), vm(2, 16, 256), vm(2, 3, 8, 128), vm(2, 3, 8, 128),
            pltpu.SMEM((1, 2), jnp.int32), vm(GY, 1, 128),
            dma((3,)),
            dma((7,)), dma((8,)), dma((7,)), dma((8,)), dma((7,)), dma((8,)), dma((7,)), dma((8,)),
            dma((4,)), dma((4,)), dma((7,)), dma((8,)), pltpu.SemaphoreType.REGULAR,
        ],
        compiler_params=pltpu.CompilerParams(collective_id=0, has_side_effects=True),
        name="amr_step",
    )(coarse_state, fine_state.reshape(NV, 32, 512), slot_site, box_live)
    coarse_out, fine_out = pl.pallas_call(
        write_out,
        out_shape=(
            jax.ShapeDtypeStruct((NV, 32, 256), F32),
            jax.ShapeDtypeStruct((NV, 32, 512), F32),
        ),
        in_specs=[pl.BlockSpec(memory_space=pl.ANY)] * 2,
        out_specs=[pl.BlockSpec(memory_space=pl.ANY)] * 2,
        scratch_shapes=[dma((2,))],
        name="write_out",
    )(*[pltpu.with_memory_space_constraint(a, pltpu.VMEM) for a in (coarse_out, fine_out)])
    return coarse_out, fine_out.reshape(1, NV, 32, 512)


def solution(mesh):
    return jax.shard_map(
        shards,
        mesh=mesh,
        in_specs=(
            P(None, "gx", "gy"),
            P(("gx", "gy"), None, None, None),
            P(("gx", "gy"), None),
            P(("gx", "gy")),
        ),
        out_specs=(P(None, "gx", "gy"), P(("gx", "gy"), None, None, None)),
        check_vma=False,
    )
```
